32 devices in a mesh: liq: 8 (over y, x, core), dur: 4 (over z).
Axes of the slice: x: 2, y: 2, z: 4, core: 2. Of those that a mesh axis runs over, the one named last changes fastest.
Arguments:
- value: float32 [128, 128, 256], P('liq', 'dur'), may hold values from -6 to 6
- utility: float32 [128, 128, 256], P('liq', 'dur'), may hold values from -6 to 6
- liq_rates: float32 [2, 128, 128, 256], P(None, 'liq', 'dur'), may hold values from 16 to 256
- dur_rates: float32 [2, 128, 128, 256], P(None, 'liq', 'dur'), may hold values from 16 to 256
- upwind: int32 [128, 128, 256], P('liq', 'dur'), may hold values from 5 to 15, as said below
- income_rates: float32 [256, 256], replicated, may hold values from -0.9 to 0.9, as said below
Outputs:
- value_next: float32 [128, 128, 256], P('liq', 'dur')
- hjb_residual: float32 [128, 128, 256], P('liq', 'dur')
The draws below stay inside these ranges and needn't reach their ends.
Inputs may be any that keep to these rules, and one draw needn't show every extreme that they name: upwind % 4 is the liquid code and upwind // 4 the durable code; a code 1 couples a cell to the next cell, 2 to the previous one, 3 to both. `income_rates`: off-diagonal entries are nonnegative, each row sums to zero, and each row's off-diagonal sum lies between 0.3 and 0.9.
All inputs are finite; a program needn't handle non-finite values.
Results may differ from the reference program's by a relative error of at most 0.0003.
Values sent between devices are 32-bit elements; how exact they have to be, the bound alone decides.
No kernel may reach another device: no remote copies, remote signals or barrier semaphores. Data moves between devices by JAX's collectives and lax.ppermute only.
A program may use at most 64 MiB of HBM per device.

```python
import math
import jax
import jax.numpy as jnp
from jax import lax

NZ = 256
STEPS = 2
NA = 128
NB = 128


def draw_upwind(key, part):
    first, second, third, fourth = jax.random.split(jax.random.fold_in(key, 11), 4)
    liq_kink = jax.random.randint(first, (1, NB, NZ), 0, NA + 1)
    dur_kink = jax.random.randint(second, (NA, 1, NZ), 0, NB + 1)
    liq_place = jnp.arange(NA).reshape(NA, 1, 1)
    dur_place = jnp.arange(NB).reshape(1, NB, 1)
    liq_code = jnp.where(liq_place < liq_kink, 1, 2)
    liq_code = jnp.where(jax.random.randint(third, (NA, NB, NZ), 0, 128) == 0, 3, liq_code)
    dur_code = jnp.where(dur_place < dur_kink, 1, 2)
    dur_code = jnp.where(jax.random.randint(fourth, (NA, NB, NZ), 0, 128) == 0, 3, dur_code)
    return (liq_code + 4 * dur_code).astype(jnp.int32)


def draw_income_rates(key, part):
    first, second = jax.random.split(jax.random.fold_in(key, 23))
    leaving = jax.random.uniform(first, (NZ, 1), jnp.float32, 0.3, 0.9)
    identity = jnp.eye(NZ, dtype=jnp.float32)
    weights = jax.random.uniform(second, (NZ, NZ), jnp.float32, 0.05, 1.0) * (1.0 - identity)
    off_part = leaving * weights / jnp.sum(weights, axis=1, keepdims=True)
    return off_part - leaving * identity


def level_of(own_key, dims, cuts, least, largest):
    def one(position, blocks):
        heights = jax.random.uniform(jax.random.fold_in(jax.random.fold_in(own_key, 6), position), (blocks,), jnp.float32, least / len(cuts), largest / len(cuts))
        return jnp.repeat(jnp.exp(heights), dims[position] // blocks).reshape((-1,) + (1,) * (len(dims) - position - 1))

    loudness = one(*cuts[0])
    for cut in cuts[1:]:
        loudness = loudness * one(*cut)
    return loudness


def normal_values(stream_key, extent, deviation, most, cuts=(), kind=jnp.bfloat16):
    drawn = deviation * jax.random.normal(stream_key, extent, jnp.float32)
    if cuts:
        drawn = drawn * level_of(stream_key, extent, cuts, -0.22, 0.18)
    return jnp.clip(drawn, -most, most).astype(kind)


def setup_inputs(seed: int = 0) -> dict:
    keys = jax.random.split(jax.random.key(seed), 7)
    value = normal_values(keys[0], (NA, NB, NZ), 1.0, 6.0, ((0, 8), (1, 4)), jnp.float32)
    utility = normal_values(keys[1], (NA, NB, NZ), 1.0, 6.0, ((0, 8), (1, 4)), jnp.float32)
    liq_rates = jnp.clip(jnp.exp(math.log(256.0) - 2.7725887 * jax.random.uniform(keys[2], (2, NA, NB, NZ), jnp.float32) ** level_of(keys[2], (2, NA, NB, NZ), ((1, 8), (2, 4)), -0.2, 0.2)), 16.0, 256.0)
    dur_rates = jnp.clip(jnp.exp(math.log(256.0) - 2.7725887 * jax.random.uniform(keys[3], (2, NA, NB, NZ), jnp.float32) ** level_of(keys[3], (2, NA, NB, NZ), ((1, 8), (2, 4)), -0.2, 0.2)), 16.0, 256.0)
    upwind = draw_upwind(jax.random.fold_in(keys[6], 71), 0)
    income_rates = draw_income_rates(jax.random.fold_in(keys[6], 71), 0)
    return dict(value=value, utility=utility, liq_rates=liq_rates, dur_rates=dur_rates, upwind=upwind, income_rates=income_rates)


DISC = 0.05


def upwind_terms(liq_rates, dur_rates, upwind, liq_first, liq_total, dur_first, dur_total):
    liq_code = upwind % 4
    dur_code = upwind // 4
    liq_place = liq_first + jnp.arange(upwind.shape[0]).astype(jnp.int32).reshape(-1, 1, 1)
    dur_place = dur_first + jnp.arange(upwind.shape[1]).astype(jnp.int32).reshape(1, -1, 1)
    liq_up = liq_rates[0] * (liq_code % 2).astype(jnp.float32) * (liq_place < liq_total - 1).astype(jnp.float32)
    liq_low = liq_rates[1] * (liq_code // 2).astype(jnp.float32) * (liq_place > 0).astype(jnp.float32)
    dur_up = dur_rates[0] * (dur_code % 2).astype(jnp.float32) * (dur_place < dur_total - 1).astype(jnp.float32)
    dur_low = dur_rates[1] * (dur_code // 2).astype(jnp.float32) * (dur_place > 0).astype(jnp.float32)
    return liq_up, liq_low, dur_up, dur_low


def income_step(field, income_rates):
    flat = field.reshape(-1, field.shape[-1])
    mixed = jnp.dot(flat, income_rates.T, precision=lax.Precision.HIGHEST, preferred_element_type=jnp.float32)
    return mixed.reshape(field.shape)


def thomas(source, upper, lower, diagonal):
    zeros = jnp.zeros_like(source[0])

    def advance(carry, cell):
        prev_offset, prev_slope = carry
        pivot = cell[3] - cell[2] * prev_slope
        new_slope = cell[1] / pivot
        new_offset = (cell[0] + cell[2] * prev_offset) / pivot
        return (new_offset, new_slope), (new_offset, new_slope)

    unused, (offset, slope) = lax.scan(advance, (zeros, zeros), (source, upper, lower, diagonal))

    def retreat(above, cell):
        here = cell[0] + cell[1] * above
        return here, here

    unused_too, solved = lax.scan(retreat, zeros, (offset, slope), reverse=True)
    return solved


def residual_of(field, padded, utility, income_rates, terms):
    liq_up, liq_low, dur_up, dur_low = terms
    result = utility + income_step(field, income_rates) - DISC * field
    result = result + liq_up * (padded[2:, 1:-1] - field) + liq_low * (padded[:-2, 1:-1] - field)
    result = result + dur_up * (padded[1:-1, 2:] - field) + dur_low * (padded[1:-1, :-2] - field)
    return result


def reference(value, utility, liq_rates, dur_rates, upwind, income_rates):
    terms = upwind_terms(liq_rates, dur_rates, upwind, 0, NA, 0, NB)
    liq_up, liq_low, dur_up, dur_low = terms
    field = value
    for step in range(STEPS):
        source = field + income_step(field, income_rates) + utility
        middle = thomas(source, liq_up, liq_low, 1.0 + liq_up + liq_low)
        flip_up = jnp.swapaxes(dur_up, 0, 1)
        flip_low = jnp.swapaxes(dur_low, 0, 1)
        solved = thomas(jnp.swapaxes(middle, 0, 1), flip_up, flip_low, 1.0 + DISC + flip_up + flip_low)
        field = jnp.swapaxes(solved, 0, 1)
    padded = jnp.pad(field, ((1, 1), (1, 1), (0, 0)))
    return field, residual_of(field, padded, utility, income_rates, terms)
```

```python
import functools

import jax
import jax.numpy as jnp
from jax import lax
from jax.experimental import pallas as pl
from jax.experimental.pallas import tpu as pltpu
from jax.sharding import PartitionSpec as P

STEPS = 2
DISC = 0.05
F32 = jnp.float32
BF16 = jnp.bfloat16
LIMIT = 24 * 1024 * 1024


def meet(left, right):
    a1, a2, b1, c1, b2, c2 = left
    d1, d2, e1, f1, e2, f2 = right
    m = 1.0 / (1.0 - c2 * e1)
    first = (m * (d1 + e1 * a2), m * e1 * b2, m * f1)
    last = (m * (a2 + c2 * d1), m * b2, m * c2 * f1)
    joint = (
        a1 + c1 * first[0],
        d2 + e2 * last[0],
        b1 + c1 * first[1],
        c1 * first[2],
        e2 * last[1],
        f2 + e2 * last[2],
    )
    return first, last, joint


def ordered(swap, own, other):
    left = tuple(jnp.where(swap, o, w) for w, o in zip(own, other))
    right = tuple(jnp.where(swap, w, o) for w, o in zip(own, other))
    return left, right


def descend(place, groups, depth=0):
    if len(groups) == 1:
        return None, None
    swap = ((place >> depth) & 1) == 1
    joints, ours = [], None
    for k in range(0, len(groups), 2):
        left, right = ordered(swap, groups[k], groups[k + 1])
        first, last, joint = meet(left, right)
        ours = ours or (first, last)
        joints.append(joint)
    p, q = descend(place, joints, depth + 1)
    return inside(swap, ours, p, q)


def inside(swap, ours, p, q):
    first, last = ours
    f, l = first[0], last[0]
    if p is not None:
        f = f + first[1] * p + first[2] * q
        l = l + last[1] * p + last[2] * q
    else:
        p, q = jnp.zeros_like(f), jnp.zeros_like(f)
    return jnp.where(swap, l, p), jnp.where(swap, q, f)


def relation(rhs, coef):
    n = coef.shape[0]
    return (rhs[0], rhs[1], coef[n - 4], coef[n - 3], coef[n - 2], coef[n - 1])


def split(x):
    high = x.astype(BF16)
    return high, (x - high.astype(F32)).astype(BF16)


def income(field, rates):
    dims = (((1,), (1,)), ((), ()))
    fh, fl = split(field)
    rh, rl = split(rates)
    dot = functools.partial(lax.dot_general, dimension_numbers=dims, preferred_element_type=F32)
    return dot(fh, rh) + (dot(fh, rl) + dot(fl, rh))


def take_rhs(rows, source, inv, low, before, alpha):
    head, prev = None, None
    for k in range(rows):
        now = source(k) * inv[k]
        if k:
            now = now + low[k] * prev
        alpha[k] = now
        head = now if head is None else head + before[k] * now
        prev = now
    return head, prev


def take_matrix(rows, coefs, diag, inv, low, before, beta, gamma):
    b1 = q = bp = gp = None
    for k in range(rows):
        up, lo = coefs(k)
        pivot = diag + up + lo
        if k:
            pivot = pivot - lo * bp
        ip = 1.0 / pivot
        lp = lo * ip
        bp = up * ip
        gp = lp * gp if k else lp
        inv[k] = ip
        low[k] = lp
        beta[k] = bp
        gamma[k] = gp
        before[k] = q if k else jnp.ones_like(ip)
        b1 = b1 + q * gp if k else gp
        q = q * bp if k else bp
    return b1, q, gp, bp


def back(rows, alpha, beta, gamma, p, q, put):
    x = q
    for k in reversed(range(rows)):
        x = alpha[k] + beta[k] * x + gamma[k] * p
        put(k, x)


def pick(on, x):
    return jnp.where(on, x, 0.0)


def open_liq(n_liq, value, utility, rates, upwind, income_rates, inv, low, before, beta, gamma, alpha, out, field):
    place = lax.axis_index("liq")
    rows = value.shape[0]
    flat = value.shape[0] * value.shape[1], value.shape[2]

    def coefs(k):
        code = upwind[k] & 3
        up = pick((code & 1) > 0, rates[0, k])
        lo = pick(code > 1, rates[1, k])
        if k == rows - 1:
            up = pick(place < n_liq - 1, up)
        if k == 0:
            lo = pick(place > 0, lo)
        return up, lo

    b1, c1, b2, c2 = take_matrix(rows, coefs, 1.0, inv, low, before, beta, gamma)
    out[2], out[3], out[4], out[5] = b1, c1, b2, c2
    v = value[...].reshape(flat)
    s = v + income(v, income_rates[...]) + utility[...].reshape(flat)
    field[...] = s.reshape(field.shape)
    out[0], out[1] = take_rhs(rows, lambda k: field[k], inv, low, before, alpha)


LANES = 128


def stride_of(rows):
    return rows + 8


def turned_shape(slabs, rows, width):
    return (width // LANES, slabs * stride_of(rows), LANES)


def put_across(turned, k, slabs, rows, x):
    for h in range(turned.shape[0]):
        turned[h, pl.ds(k, slabs, stride=stride_of(rows)), :] = x[:, h * LANES : (h + 1) * LANES]


def get_slab(turned, slab, rows):
    parts = [turned[h, pl.ds(slab * stride_of(rows), rows), :] for h in range(turned.shape[0])]
    return jnp.concatenate(parts, axis=1)


def open_dur(n_dur, rates, upwind, inv, low, before, beta, gamma, out, ups, lows):
    place = lax.axis_index("dur")
    rows, cols = rates.shape[1], rates.shape[2]
    for k in range(rows):
        code = upwind[k] >> 2
        put_across(ups, k, cols, rows, pick((code & 1) > 0, rates[0, k]))
        put_across(lows, k, cols, rows, pick(code > 1, rates[1, k]))

    def coefs(b):
        up = get_slab(ups, b, rows)
        lo = get_slab(lows, b, rows)
        if b == cols - 1:
            up = pick(place < n_dur - 1, up)
        if b == 0:
            lo = pick(place > 0, lo)
        return up, lo

    out[0], out[1], out[2], out[3] = take_matrix(cols, coefs, 1.0 + DISC, inv, low, before, beta, gamma)


def join_core(own, other, own_coef, other_coef, out):
    swap = (lax.axis_index("liq") & 1) == 1
    left, right = ordered(swap, relation(own, own_coef), relation(other, other_coef))
    joint = meet(left, right)[2]
    for k in range(out.shape[0]):
        out[k] = joint[k]


def liq_to_dur(n_chips, *refs):
    own, other, own_coef, other_coef = refs[:4]
    chips = refs[4 : 4 + n_chips]
    chip_coefs = refs[4 + n_chips : 4 + 2 * n_chips]
    alpha, beta, gamma, inv, low, before, alpha_out, out, turned = refs[4 + 2 * n_chips :]
    place = lax.axis_index("liq")
    swap = (place & 1) == 1
    left, right = ordered(swap, relation(own, own_coef), relation(other, other_coef))
    first, last, joint = meet(left, right)
    p, q = descend(place >> 1, [relation(r, c) for r, c in zip(chips, chip_coefs)])
    p, q = inside(swap, (first, last), p, q)
    rows, cols = alpha.shape[0], alpha.shape[1]

    def put(k, x):
        put_across(turned, k, cols, rows, x)

    back(rows, alpha, beta, gamma, p, q, put)
    out[0], out[1] = take_rhs(cols, lambda b: get_slab(turned, b, rows), inv, low, before, alpha_out)


def close_dur(n_dur, parts, coefs, alpha, beta, gamma, field):
    p, q = descend(lax.axis_index("dur"), [relation(r, c) for r, c in zip(parts, coefs)])
    cols, rows = alpha.shape[0], alpha.shape[1]

    def put(b, x):
        put_across(field, b, rows, cols, x)

    back(cols, alpha, beta, gamma, p, q, put)
    return p, q


def dur_to_liq(n_dur, *refs):
    parts, coefs = refs[:n_dur], refs[n_dur : 2 * n_dur]
    alpha, beta, gamma, utility, income_rates, inv, low, before, alpha_out, out, field, source = refs[2 * n_dur :]
    close_dur(n_dur, parts, coefs, alpha, beta, gamma, field)
    rows, cols = utility.shape[0], utility.shape[1]
    v = jnp.concatenate([get_slab(field, k, cols) for k in range(rows)], axis=0)
    source[...] = v + income(v, income_rates[...]) + utility[...].reshape(v.shape)
    out[0], out[1] = take_rhs(rows, lambda k: source[pl.ds(k * cols, cols), :], inv, low, before, alpha_out)


def close(n_dur, *refs):
    parts, coefs = refs[:n_dur], refs[n_dur : 2 * n_dur]
    alpha, beta, gamma, value, edges, sides, field = refs[2 * n_dur :]
    p, q = close_dur(n_dur, parts, coefs, alpha, beta, gamma, field)
    sides[0], sides[1] = p, q
    for k in range(value.shape[0]):
        value[k] = get_slab(field, k, value.shape[1])
    edges[0] = value[0]
    edges[1] = value[value.shape[0] - 1]


def residual(n_liq, n_dur, value, utility, liq_rates, dur_rates, upwind, income_rates, sides, near, far, out, acc):
    rows, cols, width = value.shape
    liq, dur = lax.axis_index("liq"), lax.axis_index("dur")
    v = value[...].reshape(rows * cols, width)
    acc[...] = income(v, income_rates[...]) - DISC * v + utility[...].reshape(v.shape)
    at = lax.broadcasted_iota(jnp.int32, (cols, width), 0)
    odd = (liq & 1) == 1
    below = jnp.where(odd, near[1], far[1])
    above = jnp.where(odd, far[0], near[0])
    for k in range(rows):
        here = value[k]
        code = upwind[k]
        lup = pick((code & 1) > 0, liq_rates[0, k])
        llo = pick((code & 2) > 0, liq_rates[1, k])
        dup = pick((code & 4) > 0, dur_rates[0, k])
        dlo = pick((code & 8) > 0, dur_rates[1, k])
        up = value[k + 1] if k < rows - 1 else jnp.where(liq < n_liq - 1, above, here)
        lo = value[k - 1] if k else jnp.where(liq > 0, below, here)
        right = jnp.where(
            at == cols - 1,
            jnp.where(dur < n_dur - 1, jnp.broadcast_to(sides[1, pl.ds(k, 1), :], here.shape), here),
            pltpu.roll(here, cols - 1, axis=0),
        )
        left = jnp.where(
            at == 0,
            jnp.where(dur > 0, jnp.broadcast_to(sides[0, pl.ds(k, 1), :], here.shape), here),
            pltpu.roll(here, 1, axis=0),
        )
        here_sum = lup * (up - here) + llo * (lo - here) + dup * (right - here) + dlo * (left - here)
        out[k] = acc[pl.ds(k * cols, cols), :] + here_sum


def call(body, outs, scratch=(), cost=1 << 20):
    def run(*args):
        return pl.pallas_call(
            body,
            out_shape=[jax.ShapeDtypeStruct(s, F32) for s in outs],
            in_specs=[pl.BlockSpec(memory_space=pltpu.VMEM)] * len(args),
            out_specs=[pl.BlockSpec(memory_space=pltpu.VMEM)] * len(outs),
            scratch_shapes=[pltpu.VMEM(s, F32) for s in scratch],
            compiler_params=pltpu.CompilerParams(vmem_limit_bytes=LIMIT),
            cost_estimate=pl.CostEstimate(flops=cost, bytes_accessed=cost, transcendentals=0),
        )(*args)

    return run


def pairs(n, k):
    return [(i, i ^ k) for i in range(n)]


def shards(n_liq, n_dur, value, utility, liq_rates, dur_rates, upwind, income_rates):
    rows, cols, width = value.shape
    cube, turned = (rows, cols, width), (cols, rows, width)
    flat = (rows * cols, width)
    across_dur, across_liq = turned_shape(cols, rows, width), turned_shape(rows, cols, width)
    swap_liq = lambda x, k: lax.ppermute(x, "liq", pairs(n_liq, k))
    swap_dur = lambda x, k: lax.ppermute(x, "dur", pairs(n_dur, k))
    n_chips = n_liq // 2
    l_inv, l_low, l_before, l_beta, l_gamma, alpha, mine = call(
        functools.partial(open_liq, n_liq), [cube] * 6 + [(6, cols, width)], [cube]
    )(value, utility, liq_rates, upwind, income_rates)
    d_inv, d_low, d_before, d_beta, d_gamma, d_mine = call(
        functools.partial(open_dur, n_dur), [turned] * 5 + [(4, rows, width)], [across_dur] * 2
    )(dur_rates, upwind)
    d_coefs = [d_mine] + [swap_dur(d_mine, k) for k in range(1, n_dur)]
    own_coef = other_coef = chip_coefs = None
    for step in range(STEPS):
        other = swap_liq(mine, 1)
        if step == 0:
            own_coef, other_coef = mine, other
        (joint,) = call(join_core, [(6 if step == 0 else 2, cols, width)])(mine, other, own_coef, other_coef)
        chips = [joint] + [swap_liq(joint, 2 * k) for k in range(1, n_chips)]
        if step == 0:
            chip_coefs = chips
        d_alpha, d_rhs = call(functools.partial(liq_to_dur, n_chips), [turned, (2, rows, width)], [across_dur])(
            mine, other, own_coef, other_coef, *chips, *chip_coefs, alpha, l_beta, l_gamma, d_inv, d_low, d_before
        )
        parts = [d_rhs] + [swap_dur(d_rhs, k) for k in range(1, n_dur)]
        if step < STEPS - 1:
            alpha, mine = call(functools.partial(dur_to_liq, n_dur), [cube, (2, cols, width)], [across_liq, flat])(
                *parts, *d_coefs, d_alpha, d_beta, d_gamma, utility, income_rates, l_inv, l_low, l_before
            )
    field, edges, sides = call(functools.partial(close, n_dur), [cube, (2, cols, width), (2, rows, width)], [across_liq])(
        *parts, *d_coefs, d_alpha, d_beta, d_gamma
    )
    near = swap_liq(edges, 1)
    between = [(i, i + 1) for i in range(1, n_liq - 1, 2)]
    far = lax.ppermute(edges, "liq", between + [(j, i) for i, j in between])
    (result,) = call(functools.partial(residual, n_liq, n_dur), [cube], [flat])(
        field, utility, liq_rates, dur_rates, upwind, income_rates, sides, near, far
    )
    return field, result


def solution(mesh):
    n_liq, n_dur = mesh.shape["liq"], mesh.shape["dur"]
    cell = P("liq", "dur", None)
    pair = P(None, "liq", "dur", None)
    return jax.shard_map(
        functools.partial(shards, n_liq, n_dur),
        mesh=mesh,
        in_specs=(cell, cell, pair, pair, cell, P()),
        out_specs=(cell, cell),
        check_vma=False,
    )
```

```python
import functools

import jax
import jax.numpy as jnp
from jax import lax
from jax.experimental import pallas as pl
from jax.experimental.pallas import tpu as pltpu
from jax.sharding import PartitionSpec as P


STEPS = 2
DISC = 0.05
F32 = jnp.float32
BF16 = jnp.bfloat16
LIMIT = 24 * 1024 * 1024
OPEN_LIMIT = 50 * 1024 * 1024


def meet(left, right):
    a1, a2, b1, c1, b2, c2 = left
    d1, d2, e1, f1, e2, f2 = right
    m = 1.0 / (1.0 - c2 * e1)
    first = (m * (d1 + e1 * a2), m * e1 * b2, m * f1)
    last = (m * (a2 + c2 * d1), m * b2, m * c2 * f1)
    joint = (
        a1 + c1 * first[0],
        d2 + e2 * last[0],
        b1 + c1 * first[1],
        c1 * first[2],
        e2 * last[1],
        f2 + e2 * last[2],
    )
    return first, last, joint


def ordered(swap, own, other):
    left = tuple(jnp.where(swap, o, w) for w, o in zip(own, other))
    right = tuple(jnp.where(swap, w, o) for w, o in zip(own, other))
    return left, right


def descend(place, groups, depth=0):
    if len(groups) == 1:
        return None, None
    swap = ((place >> depth) & 1) == 1
    joints, ours = [], None
    for k in range(0, len(groups), 2):
        left, right = ordered(swap, groups[k], groups[k + 1])
        first, last, joint = meet(left, right)
        ours = ours or (first, last)
        joints.append(joint)
    p, q = descend(place, joints, depth + 1)
    return inside(swap, ours, p, q)


def inside(swap, ours, p, q):
    first, last = ours
    f, l = first[0], last[0]
    if p is not None:
        f = f + first[1] * p + first[2] * q
        l = l + last[1] * p + last[2] * q
    else:
        p, q = jnp.zeros_like(f), jnp.zeros_like(f)
    return jnp.where(swap, l, p), jnp.where(swap, q, f)


def relation(rhs, coef, at):
    part = pl.ds(0, rhs.shape[1])
    return (rhs[0], rhs[1], *(coef[k, part] for k in range(at, at + 4)))


def split(x):
    high = x.astype(BF16)
    return high, (x - high.astype(F32)).astype(BF16)


def income(field, high, low):
    dims = (((1,), (1,)), ((), ()))
    fh, fl = split(field)
    rh, rl = high[...], low[...]
    dot = functools.partial(lax.dot_general, dimension_numbers=dims, preferred_element_type=F32)
    return dot(fh, rh) + (dot(fh, rl) + dot(fl, rh))


def take_rhs(rows, source, inv, low, before, alpha):
    head, prev = None, None
    for k in range(rows):
        now = source(k)
        part = pl.ds(0, now.shape[0])
        now = now * inv[k, part]
        if k:
            now = now + low[k, part] * prev
        alpha[k] = now
        head = now if head is None else head + before[k, part] * now
        prev = now
    return head, prev


def take_matrix(rows, coefs, diag, inv, low, before, beta, gamma):
    b1 = q = bp = gp = None
    for k in range(rows):
        up, lo = coefs(k)
        pivot = diag + up + lo
        if k:
            pivot = pivot - lo * bp
        ip = 1.0 / pivot
        lp = lo * ip
        bp = up * ip
        gp = lp * gp if k else lp
        inv[k] = ip
        low[k] = lp
        beta[k] = bp
        gamma[k] = gp
        before[k] = q if k else jnp.ones_like(ip)
        b1 = b1 + q * gp if k else gp
        q = q * bp if k else bp
    return b1, q, gp, bp


def back(rows, alpha, beta, gamma, p, q, put):
    x = q
    part = pl.ds(0, x.shape[0])
    for k in reversed(range(rows)):
        x = alpha[k] + beta[k, part] * x + gamma[k, part] * p
        put(k, x)


def pick(on, x):
    return jnp.where(on, x, 0.0)


LANES = 128


def stride_of(rows):
    return rows if rows % 16 else rows + 8


def turned_shape(slabs, rows, width):
    return (width // LANES, slabs * stride_of(rows), LANES)


def put_across(turned, k, slabs, rows, x):
    for h in range(turned.shape[0]):
        turned[h, pl.ds(k, slabs, stride=stride_of(rows)), :] = x[:, h * LANES : (h + 1) * LANES]


def get_slab(turned, slab, rows):
    parts = [turned[h, pl.ds(slab * stride_of(rows), rows), :] for h in range(turned.shape[0])]
    return jnp.concatenate(parts, axis=1)


def fetch(pairs, sems):
    copies = [pltpu.make_async_copy(src, dst, sems.at[k]) for k, (src, dst) in enumerate(pairs)]
    for copy in copies:
        copy.start()
    return copies


def open_liq(n_liq, rates_h, dur_rates_h, upwind_h, *refs):
    inv, low, before, beta, gamma, out, ups, lows, far = refs[:9]
    rates, edges, upwind, sems = refs[9:]
    rows = upwind.shape[0]
    copies = fetch(
        [
            (rates_h, rates),
            (upwind_h, upwind),
            (dur_rates_h.at[:, 0], edges.at[0]),
            (dur_rates_h.at[:, rows - 1], edges.at[1]),
        ],
        sems,
    )
    place = lax.axis_index("liq")

    def coefs(k):
        code = upwind[k]
        up = pick((code & 1) > 0, rates[0, k])
        lo = pick((code & 2) > 0, rates[1, k])
        if k == rows - 1:
            up = pick(place < n_liq - 1, up)
        if k == 0:
            lo = pick(place > 0, lo)
        ups[k], lows[k] = up, lo
        return up, lo

    for copy in copies:
        copy.wait()
    out[0], out[1], out[2], out[3] = take_matrix(rows, coefs, 1.0, inv, low, before, beta, gamma)
    odd = (place & 1) == 1
    for k in range(2):
        head = pick((upwind[0] & (4 << k)) > 0, edges[0, k])
        tail = pick((upwind[rows - 1] & (4 << k)) > 0, edges[1, k])
        out[4 + k] = jnp.where(odd, head, tail)
        far[k] = jnp.where(odd, tail, head)


def open_source(value, utility, income_rates, coef, inv, low, before, alpha, out, high, less, source):
    rows, cols, width = value.shape
    v = value[...].reshape(rows * cols, width)
    high[...], less[...] = split(income_rates[...])
    source[...] = v + income(v, high, less) + utility[...].reshape(v.shape)
    out[0], out[1] = take_rhs(rows, lambda k: source[pl.ds(k * cols, cols), :], inv, low, before, alpha)
    for k in range(coef.shape[0]):
        out[2 + k] = coef[k]


EXTRA = 8


def open_dur(n_dur, rates, upwind, near, far, inv, low, before, beta, gamma, out, ups, lows):
    place = lax.axis_index("dur")
    odd = (lax.axis_index("liq") & 1) == 1
    rows, cols = rates.shape[1], rates.shape[2]
    wide = rows + EXTRA
    for j, turned in enumerate((ups, lows)):
        for k in range(rows):
            put_across(turned, k, cols, wide, pick((upwind[k] & (4 << j)) > 0, rates[j, k]))
        put_across(turned, rows, cols, wide, jnp.where(odd, near[6 + j], far[j]))
        put_across(turned, rows + 1, cols, wide, jnp.where(odd, far[j], near[6 + j]))
        for k in range(rows + 2, wide):
            put_across(turned, k, cols, wide, jnp.zeros_like(far[j]))

    def coefs(b):
        up, lo = get_slab(ups, b, wide), get_slab(lows, b, wide)
        if b == cols - 1:
            up = pick(place < n_dur - 1, up)
        if b == 0:
            lo = pick(place > 0, lo)
        return up, lo

    out[0], out[1], out[2], out[3] = take_matrix(cols, coefs, 1.0 + DISC, inv, low, before, beta, gamma)


def join_core(own, other, own_coef, other_coef, out):
    swap = (lax.axis_index("liq") & 1) == 1
    left, right = ordered(swap, relation(own, own_coef, 2), relation(other, other_coef, 2))
    joint = meet(left, right)[2]
    for k in range(out.shape[0]):
        out[k] = joint[k]


def liq_to_dur(n_chips, *refs):
    own, other, own_coef, other_coef = refs[:4]
    chips = refs[4 : 4 + n_chips]
    chip_coefs = refs[4 + n_chips : 4 + 2 * n_chips]
    alpha, beta, gamma, inv, low, before, alpha_out, out, turned = refs[4 + 2 * n_chips :]
    place = lax.axis_index("liq")
    swap = (place & 1) == 1
    left, right = ordered(swap, relation(own, own_coef, 2), relation(other, other_coef, 2))
    first, last, _ = meet(left, right)
    p, q = descend(place >> 1, [relation(r, c, 2) for r, c in zip(chips, chip_coefs)])
    p, q = inside(swap, (first, last), p, q)
    rows, cols = alpha.shape[0], alpha.shape[1]
    wide, taken = rows + EXTRA, alpha_out.shape[1]
    if taken > rows:
        put_across(turned, rows, cols, wide, p)
        put_across(turned, rows + 1, cols, wide, q)
        for k in range(rows + 2, wide):
            put_across(turned, k, cols, wide, jnp.zeros_like(p))
    back(rows, alpha, beta, gamma, p, q, lambda k, x: put_across(turned, k, cols, wide, x))
    out[0], out[1] = take_rhs(
        cols, lambda b: get_slab(turned, b, wide)[:taken], inv, low, before, alpha_out
    )


def beside_dur(parts, coefs):
    return descend(lax.axis_index("dur"), [relation(r, c, 0) for r, c in zip(parts, coefs)])


def dur_to_liq(n_dur, *refs):
    parts, coefs = refs[:n_dur], refs[n_dur : 2 * n_dur]
    alpha, beta, gamma, utility, high, less, inv, low, before, alpha_out, out, field, source = refs[2 * n_dur :]
    p, q = beside_dur(parts, coefs)
    rows, cols = utility.shape[0], utility.shape[1]
    back(cols, alpha, beta, gamma, p, q, lambda b, x: put_across(field, b, rows, cols, x))
    v = jnp.concatenate([get_slab(field, k, cols) for k in range(rows)], axis=0)
    source[...] = v + income(v, high, less) + utility[...].reshape(v.shape)
    out[0], out[1] = take_rhs(rows, lambda k: source[pl.ds(k * cols, cols), :], inv, low, before, alpha_out)


def close(n_liq, n_dur, *refs):
    parts, coefs = refs[:n_dur], refs[n_dur : 2 * n_dur]
    alpha, beta, gamma, utility, high, less, liq_ups, liq_lows, dur_ups, dur_lows = refs[2 * n_dur : 2 * n_dur + 10]
    value_h, out_h, field, drift, value, out, sems = refs[2 * n_dur + 10 :]
    rows, cols, width = utility.shape
    wide = alpha.shape[1]
    liq, dur = lax.axis_index("liq"), lax.axis_index("dur")
    p, q = beside_dur(parts, coefs)
    after, here = jnp.where(dur < n_dur - 1, q, 0.0)[:rows], None
    x = q

    def flow(b, here, after, ahead):
        up, lo = get_slab(dur_ups, b, wide)[:rows], get_slab(dur_lows, b, wide)[:rows]
        if b == cols - 1:
            up = pick(dur < n_dur - 1, up)
        if b == 0:
            lo = pick(dur > 0, lo)
        put_across(drift, b, rows, cols, up * (after - here) + lo * (ahead - here))

    for b in reversed(range(cols)):
        x = alpha[b] + beta[b] * x + gamma[b] * p
        put_across(field, b, rows + 2, cols, x[: rows + 2])
        now = x[:rows]
        if here is not None:
            flow(b + 1, here, after, now)
            after = here
        here = now
    flow(0, here, after, p[:rows])
    for k in range(rows):
        value[k] = get_slab(field, k, cols)
    saved = pltpu.make_async_copy(value, value_h, sems.at[0])
    saved.start()
    v = value[...].reshape(rows * cols, width)
    out[...] = (income(v, high, less) - DISC * v).reshape(out.shape) + utility[...]
    parts = 4
    sent = []
    for k in range(rows):
        here = value[k]
        up = value[k + 1] if k < rows - 1 else jnp.where(liq < n_liq - 1, get_slab(field, rows + 1, cols), here)
        lo = value[k - 1] if k else jnp.where(liq > 0, get_slab(field, rows, cols), here)
        moved = liq_ups[k] * (up - here) + liq_lows[k] * (lo - here) + get_slab(drift, k, cols)
        out[k] = out[k] + moved
        if (k + 1) % (rows // parts) == 0:
            piece = pl.ds(k + 1 - rows // parts, rows // parts)
            sent.append(pltpu.make_async_copy(out.at[piece], out_h.at[piece], sems.at[1 + len(sent)]))
            sent[-1].start()
    saved.wait()
    for copy in sent:
        copy.wait()


def call(body, outs, scratch=(), sems=0, cost=1 << 20, ins=pltpu.VMEM, to=pltpu.VMEM, limit=LIMIT):
    def run(*args):
        return pl.pallas_call(
            body,
            out_shape=[jax.ShapeDtypeStruct(s, F32) if isinstance(s, tuple) else s for s in outs],
            in_specs=[pl.BlockSpec(memory_space=ins)] * len(args),
            out_specs=[pl.BlockSpec(memory_space=to)] * len(outs),
            scratch_shapes=[s if not isinstance(s, tuple) else pltpu.VMEM(s, F32) for s in scratch]
            + ([pltpu.SemaphoreType.DMA((sems,))] if sems else []),
            compiler_params=pltpu.CompilerParams(vmem_limit_bytes=limit),
            cost_estimate=pl.CostEstimate(flops=cost, bytes_accessed=cost, transcendentals=0),
        )(*args)

    return run


def pairs(n, k):
    return [(i, i ^ k) for i in range(n)]


def shards(n_liq, n_dur, value, utility, liq_rates, dur_rates, upwind, income_rates):
    rows, cols, width = value.shape
    wide = rows + EXTRA
    cube, turned, flat = (rows, cols, width), (cols, wide, width), (rows * cols, width)
    across_dur, across_liq = turned_shape(cols, wide, width), turned_shape(rows, cols, width)
    swap_liq = lambda x, k: lax.ppermute(x, "liq", pairs(n_liq, k))
    swap_dur = lambda x, k: lax.ppermute(x, "dur", pairs(n_dur, k))
    n_chips = n_liq // 2
    l_inv, l_low, l_before, l_beta, l_gamma, own, liq_ups, liq_lows, far = call(
        functools.partial(open_liq, n_liq),
        [cube] * 5 + [(6, cols, width)] + [cube] * 2 + [(2, cols, width)],
        [(2, *cube), (2, 2, cols, width), pltpu.VMEM(cube, jnp.int32)],
        sems=4,
        ins=pltpu.HBM,
        limit=OPEN_LIMIT,
    )(liq_rates, dur_rates, upwind)
    alpha, mine, high, less = call(
        open_source, [cube, (8, cols, width)] + [jax.ShapeDtypeStruct((width, width), BF16)] * 2, [flat]
    )(value, utility, income_rates, own, l_inv, l_low, l_before)
    between = [(i, i + 1) for i in range(1, n_liq - 1, 2)]
    far = lax.ppermute(far, "liq", between + [(j, i) for i, j in between])
    own_coef = other_coef = chip_coefs = None
    for step in range(STEPS):
        other = swap_liq(mine, 1)
        if step == 0:
            own_coef, other_coef = mine, other
        (joint,) = call(join_core, [(6 if step == 0 else 2, cols, width)])(mine, other, own_coef, other_coef)
        chips = [joint] + [swap_liq(joint, 2 * k) for k in range(1, n_chips)]
        if step == 0:
            chip_coefs = chips
            d_inv, d_low, d_before, d_beta, d_gamma, d_mine, dur_ups, dur_lows = call(
                functools.partial(open_dur, n_dur), [turned] * 5 + [(4, wide, width)] + [across_dur] * 2
            )(dur_rates, upwind, other, far)
            d_coefs = [d_mine] + [swap_dur(d_mine, k) for k in range(1, n_dur)]
        taken = rows if step < STEPS - 1 else wide
        d_alpha, d_rhs = call(
            functools.partial(liq_to_dur, n_chips), [(cols, taken, width), (2, taken, width)], [across_dur]
        )(mine, other, own_coef, other_coef, *chips, *chip_coefs, alpha, l_beta, l_gamma, d_inv, d_low, d_before)
        parts = [d_rhs] + [swap_dur(d_rhs, k) for k in range(1, n_dur)]
        if step < STEPS - 1:
            alpha, mine = call(functools.partial(dur_to_liq, n_dur), [cube, (2, cols, width)], [across_liq, flat])(
                *parts, *d_coefs, d_alpha, d_beta, d_gamma, utility, high, less, l_inv, l_low, l_before
            )
    return call(
        functools.partial(close, n_liq, n_dur),
        [cube, cube],
        [turned_shape(rows + 2, cols, width), across_liq, cube, cube],
        sems=5,
        to=pltpu.HBM,
    )(*parts, *d_coefs, d_alpha, d_beta, d_gamma, utility, high, less, liq_ups, liq_lows, dur_ups, dur_lows)


def solution(mesh):
    n_liq, n_dur = mesh.shape["liq"], mesh.shape["dur"]
    cell = P("liq", "dur", None)
    pair = P(None, "liq", "dur", None)

    def body(*args):
        return shards(n_liq, n_dur, *args)

    return jax.shard_map(
        body,
        mesh=mesh,
        in_specs=(cell, cell, pair, pair, cell, P()),
        out_specs=(cell, cell),
        check_vma=False,
    )
```

```python
import functools

import jax
import jax.numpy as jnp
from jax import lax
from jax.experimental import pallas as pl
from jax.experimental.pallas import tpu as pltpu
from jax.sharding import PartitionSpec as P


STEPS = 2
DISC = 0.05
F32 = jnp.float32
BF16 = jnp.bfloat16
LIMIT = 24 * 1024 * 1024
OPEN_LIMIT = 50 * 1024 * 1024


def meet(left, right):
    a1, a2, b1, c1, b2, c2 = left
    d1, d2, e1, f1, e2, f2 = right
    m = 1.0 / (1.0 - c2 * e1)
    first = (m * (d1 + e1 * a2), m * e1 * b2, m * f1)
    last = (m * (a2 + c2 * d1), m * b2, m * c2 * f1)
    joint = (
        a1 + c1 * first[0],
        d2 + e2 * last[0],
        b1 + c1 * first[1],
        c1 * first[2],
        e2 * last[1],
        f2 + e2 * last[2],
    )
    return first, last, joint


def ordered(swap, own, other):
    left = tuple(jnp.where(swap, o, w) for w, o in zip(own, other))
    right = tuple(jnp.where(swap, w, o) for w, o in zip(own, other))
    return left, right


def descend(place, groups, depth=0):
    if len(groups) == 1:
        return None, None
    swap = ((place >> depth) & 1) == 1
    joints, ours = [], None
    for k in range(0, len(groups), 2):
        left, right = ordered(swap, groups[k], groups[k + 1])
        first, last, joint = meet(left, right)
        ours = ours or (first, last)
        joints.append(joint)
    p, q = descend(place, joints, depth + 1)
    return inside(swap, ours, p, q)


def inside(swap, ours, p, q):
    first, last = ours
    f, l = first[0], last[0]
    if p is not None:
        f = f + first[1] * p + first[2] * q
        l = l + last[1] * p + last[2] * q
    else:
        p, q = jnp.zeros_like(f), jnp.zeros_like(f)
    return jnp.where(swap, l, p), jnp.where(swap, q, f)


def relation(rhs, coef, at):
    part = pl.ds(0, rhs.shape[1])
    return (rhs[0], rhs[1], *(coef[k, part] for k in range(at, at + 4)))


def split(x):
    high = x.astype(BF16)
    return high, (x - high.astype(F32)).astype(BF16)


def income(field, high, low):
    dims = (((1,), (1,)), ((), ()))
    fh, fl = split(field)
    rh, rl = high[...], low[...]
    dot = functools.partial(lax.dot_general, dimension_numbers=dims, preferred_element_type=F32)
    return dot(fh, rh) + (dot(fh, rl) + dot(fl, rh))


def take_rhs(rows, source, inv, low, before, alpha):
    head, prev = None, None
    for k in range(rows):
        now = source(k)
        part = pl.ds(0, now.shape[0])
        now = now * inv[k, part]
        if k:
            now = now + low[k, part] * prev
        alpha[k] = now
        head = now if head is None else head + before[k, part] * now
        prev = now
    return head, prev


def take_matrix(rows, coefs, diag, inv, low, before, beta, gamma):
    b1 = q = bp = gp = None
    for k in range(rows):
        up, lo = coefs(k)
        pivot = diag + up + lo
        if k:
            pivot = pivot - lo * bp
        ip = 1.0 / pivot
        lp = lo * ip
        bp = up * ip
        gp = lp * gp if k else lp
        inv[k] = ip
        low[k] = lp
        beta[k] = bp
        gamma[k] = gp
        before[k] = q if k else jnp.ones_like(ip)
        b1 = b1 + q * gp if k else gp
        q = q * bp if k else bp
    return b1, q, gp, bp


def back(rows, alpha, beta, gamma, p, q, put):
    x = q
    part = pl.ds(0, x.shape[0])
    for k in reversed(range(rows)):
        x = alpha[k] + beta[k, part] * x + gamma[k, part] * p
        put(k, x)


def pick(on, x):
    return jnp.where(on, x, 0.0)


LANES = 128


def stride_of(rows):
    return rows if rows % 16 else rows + 8


def turned_shape(slabs, rows, width):
    return (width // LANES, slabs * stride_of(rows), LANES)


def put_across(turned, k, slabs, rows, x, first=0):
    stride = stride_of(rows)
    for h in range(turned.shape[0]):
        turned[h, pl.ds(first * stride + k, slabs, stride=stride), :] = x[:, h * LANES : (h + 1) * LANES]


def get_slab(turned, slab, rows):
    parts = [turned[h, pl.ds(slab * stride_of(rows), rows), :] for h in range(turned.shape[0])]
    return jnp.concatenate(parts, axis=1)


def fetch(pairs, sems):
    copies = [pltpu.make_async_copy(src, dst, sems.at[k]) for k, (src, dst) in enumerate(pairs)]
    for copy in copies:
        copy.start()
    return copies


def open_liq(n_liq, rates_h, dur_rates_h, upwind_h, *refs):
    inv, low, before, beta, gamma, out, ups, lows, far = refs[:9]
    rates, edges, upwind, sems = refs[9:]
    rows = upwind.shape[0]
    copies = fetch(
        [
            (rates_h, rates),
            (upwind_h, upwind),
            (dur_rates_h.at[:, 0], edges.at[0]),
            (dur_rates_h.at[:, rows - 1], edges.at[1]),
        ],
        sems,
    )
    place = lax.axis_index("liq")

    def coefs(k):
        code = upwind[k]
        up = pick((code & 1) > 0, rates[0, k])
        lo = pick((code & 2) > 0, rates[1, k])
        if k == rows - 1:
            up = pick(place < n_liq - 1, up)
        if k == 0:
            lo = pick(place > 0, lo)
        ups[k], lows[k] = up, lo
        return up, lo

    for copy in copies:
        copy.wait()
    out[0], out[1], out[2], out[3] = take_matrix(rows, coefs, 1.0, inv, low, before, beta, gamma)
    odd = (place & 1) == 1
    for k in range(2):
        head = pick((upwind[0] & (4 << k)) > 0, edges[0, k])
        tail = pick((upwind[rows - 1] & (4 << k)) > 0, edges[1, k])
        out[4 + k] = jnp.where(odd, head, tail)
        far[k] = jnp.where(odd, tail, head)


def open_source(value, utility, income_rates, coef, inv, low, before, alpha, out, high, less, source):
    rows, cols, width = value.shape
    v = value[...].reshape(rows * cols, width)
    high[...], less[...] = split(income_rates[...])
    source[...] = v + income(v, high, less) + utility[...].reshape(v.shape)
    out[0], out[1] = take_rhs(rows, lambda k: source[pl.ds(k * cols, cols), :], inv, low, before, alpha)
    for k in range(coef.shape[0]):
        out[2 + k] = coef[k]


def open_dur(n_dur, rates, upwind, inv, low, before, beta, gamma, out, ups, lows):
    rows, cols = rates.shape[1], rates.shape[2]
    for j, turned in enumerate((ups, lows)):
        for k in range(rows):
            put_across(turned, k, cols, rows, pick((upwind[k] & (4 << j)) > 0, rates[j, k]))
    coefs = dur_coefs(n_dur, cols, rows, ups, lows)
    out[0], out[1], out[2], out[3] = take_matrix(cols, coefs, 1.0 + DISC, inv, low, before, beta, gamma)


def dur_coefs(n_dur, cols, rows, ups, lows):
    place = lax.axis_index("dur")

    def coefs(b):
        up, lo = get_slab(ups, b, rows), get_slab(lows, b, rows)
        if b == cols - 1:
            up = pick(place < n_dur - 1, up)
        if b == 0:
            lo = pick(place > 0, lo)
        return up, lo

    return coefs


EDGE = 8


def put_edges(turned, cols, previous, following):
    put_across(turned, 0, cols, EDGE, previous)
    put_across(turned, 1, cols, EDGE, following)
    for k in range(2, EDGE):
        put_across(turned, k, cols, EDGE, jnp.zeros_like(previous))


def open_edge(n_dur, near, far, inv, low, before, beta, gamma, out, ups, lows):
    odd = (lax.axis_index("liq") & 1) == 1
    cols = inv.shape[0]
    for j, turned in enumerate((ups, lows)):
        put_edges(turned, cols, jnp.where(odd, near[6 + j], far[j]), jnp.where(odd, far[j], near[6 + j]))
    coefs = dur_coefs(n_dur, cols, EDGE, ups, lows)
    matrix = take_matrix(cols, coefs, 1.0 + DISC, inv, low, before, beta, gamma)
    out[...] = jnp.concatenate([m[:2] for m in matrix], axis=0)


def join_core(own, other, own_coef, other_coef, out, *half):
    swap = (lax.axis_index("liq") & 1) == 1
    left, right = ordered(swap, relation(own, own_coef, 2), relation(other, other_coef, 2))
    joint = meet(left, right)[2]
    for k in range(out.shape[0]):
        out[k] = joint[k]
    for part in half:
        lines = part.shape[1]
        for k in range(out.shape[0]):
            part[k] = jnp.where(swap, joint[k][lines:], joint[k][:lines])


def mend(*refs):
    n = len(refs) // 3
    swap = (lax.axis_index("liq") & 1) == 1
    for mine, other, out in zip(refs[:n], refs[n : 2 * n], refs[2 * n :]):
        lines = mine.shape[1]
        for k in range(out.shape[0]):
            out[k, pl.ds(0, lines)] = jnp.where(swap, other[k], mine[k])
            out[k, pl.ds(lines, lines)] = jnp.where(swap, mine[k], other[k])


def liq_to_dur(n_chips, *refs):
    own, other, own_coef, other_coef = refs[:4]
    chips = refs[4 : 4 + n_chips]
    chip_coefs = refs[4 + n_chips : 4 + 2 * n_chips]
    alpha, beta, gamma, inv, low, before = refs[4 + 2 * n_chips : 10 + 2 * n_chips]
    edge = refs[10 + 2 * n_chips :]
    if len(edge) > 3:
        e_inv, e_low, e_before, e_coef, alpha_out, out, e_alpha, turned, e_turned = edge
    else:
        alpha_out, out, turned = edge
    place = lax.axis_index("liq")
    swap = (place & 1) == 1
    left, right = ordered(swap, relation(own, own_coef, 2), relation(other, other_coef, 2))
    first, last, _ = meet(left, right)
    p, q = descend(place >> 1, [relation(r, c, 2) for r, c in zip(chips, chip_coefs)])
    p, q = inside(swap, (first, last), p, q)
    rows, cols = alpha.shape[0], alpha.shape[1]
    if len(edge) > 3:
        put_edges(e_turned, cols, p, q)
        ends = take_rhs(cols, lambda b: get_slab(e_turned, b, EDGE), e_inv, e_low, e_before, e_alpha)
        out[pl.ds(2 * rows, EDGE)] = jnp.concatenate([e[:2] for e in ends + ends], axis=0)
        out[pl.ds(2 * rows + EDGE, EDGE)] = e_coef[...]
    back(rows, alpha, beta, gamma, p, q, lambda k, x: put_across(turned, k, cols, rows, x))
    ends = take_rhs(cols, lambda b: get_slab(turned, b, rows), inv, low, before, alpha_out)
    for k in range(2):
        out[pl.ds(k * rows, rows)] = ends[k]


QUAD = 4


def pair_weights(own, other, out):
    place = lax.axis_index("dur")
    swap, upper = (place & 1) == 1, (place & 2) == 2
    mine, its = (tuple(ref[k] for k in range(4)) for ref in (own, other))
    (b1, c1, b2, c2), (e1, f1, e2, f2) = ordered(swap, mine, its)
    m = 1.0 / (1.0 - c2 * e1)
    out[0] = jnp.where(upper, c1 * m * e1, e2 * m)
    out[1] = jnp.where(upper, c1 * m, e2 * m * c2)
    out[2] = jnp.where(upper, b1 + c1 * m * e1 * b2, f2 + e2 * m * c2 * f1)


def beside_dur(parts, coefs):
    place = lax.axis_index("dur")
    rows = coefs[0].shape[1]
    sides = [tuple(ref[pl.ds(k * rows, rows)] for k in range(2)) for ref in parts]
    if len(parts) != QUAD:
        return descend(place, [side + tuple(c[k] for k in range(4)) for side, c in zip(sides, coefs)])
    swap, upper = (place & 1) == 1, (place & 2) == 2
    near = [side + tuple(c[k] for k in range(4)) for side, c in zip(sides[:2], coefs[:2])]
    first, last, joint = meet(*ordered(swap, *near))
    (l1, l2), (r1, r2) = ordered(swap, *sides[2:])
    w = [coefs[2][k] for k in range(3)]
    far = jnp.where(upper, r2, l1) + w[0] * l2 + w[1] * r1
    ours = jnp.where(upper, joint[0], joint[1])
    slope = jnp.where(upper, joint[2], joint[5])
    beyond = (far + w[2] * ours) / (1.0 - w[2] * slope)
    none = jnp.zeros_like(beyond)
    return inside(swap, (first, last), jnp.where(upper, beyond, none), jnp.where(upper, none, beyond))


def beside_edge(parts, rows):
    def piece(ref, k):
        return ref[pl.ds(k, 2)]

    at = [2 * rows, 2 * rows + 2] + [2 * rows + EDGE + 2 * k for k in range(4)]
    return descend(lax.axis_index("dur"), [tuple(piece(ref, k) for k in at) for ref in parts])


def given_dur(n_dur, refs):
    coefs = 3 if n_dur == QUAD else n_dur
    return refs[:n_dur], refs[n_dur : n_dur + coefs], refs[n_dur + coefs :]


def dur_to_liq(n_dur, *refs):
    parts, coefs, refs = given_dur(n_dur, refs)
    alpha, beta, gamma, utility, high, less, inv, low, before, alpha_out, out, field, source = refs
    p, q = beside_dur(parts, coefs)
    rows, cols = utility.shape[0], utility.shape[1]
    back(cols, alpha, beta, gamma, p, q, lambda b, x: put_across(field, b, rows, cols, x))
    v = jnp.concatenate([get_slab(field, k, cols) for k in range(rows)], axis=0)
    source[...] = v + income(v, high, less) + utility[...].reshape(v.shape)
    out[0], out[1] = take_rhs(rows, lambda k: source[pl.ds(k * cols, cols), :], inv, low, before, alpha_out)


def close(n_liq, n_dur, *refs):
    parts, coefs, refs = given_dur(n_dur, refs)
    alpha, beta, gamma, e_alpha, e_beta, e_gamma = refs[:6]
    utility, high, less, liq_ups, liq_lows, dur_ups, dur_lows = refs[6:13]
    value_h, out_h, field, drift, value, out, sems = refs[13:]
    rows, cols, width = utility.shape
    liq, dur = lax.axis_index("liq"), lax.axis_index("dur")
    p, q = beside_dur(parts, coefs)
    after, here = jnp.where(dur < n_dur - 1, q, 0.0), None
    x = q
    rates = dur_coefs(n_dur, cols, rows, dur_ups, dur_lows)

    def flow(b, here, after, ahead):
        up, lo = rates(b)
        put_across(drift, b, rows, cols, up * (after - here) + lo * (ahead - here))

    for b in reversed(range(cols)):
        x = alpha[b] + beta[b] * x + gamma[b] * p
        put_across(field, b, rows, cols, x)
        if here is not None:
            flow(b + 1, here, after, x)
            after = here
        here = x
    flow(0, here, after, p)
    p, x = beside_edge(parts, rows)
    for b in reversed(range(cols)):
        x = e_alpha[b, :2] + e_beta[b, :2] * x + e_gamma[b, :2] * p
        put_across(field, b, 2, cols, x, first=rows)
    for k in range(rows):
        value[k] = get_slab(field, k, cols)
    saved = pltpu.make_async_copy(value, value_h, sems.at[0])
    saved.start()
    v = value[...].reshape(rows * cols, width)
    out[...] = (income(v, high, less) - DISC * v).reshape(out.shape) + utility[...]
    parts = 4
    sent = []
    for k in range(rows):
        here = value[k]
        up = value[k + 1] if k < rows - 1 else jnp.where(liq < n_liq - 1, get_slab(field, rows + 1, cols), here)
        lo = value[k - 1] if k else jnp.where(liq > 0, get_slab(field, rows, cols), here)
        moved = liq_ups[k] * (up - here) + liq_lows[k] * (lo - here) + get_slab(drift, k, cols)
        out[k] = out[k] + moved
        if (k + 1) % (rows // parts) == 0:
            piece = pl.ds(k + 1 - rows // parts, rows // parts)
            sent.append(pltpu.make_async_copy(out.at[piece], out_h.at[piece], sems.at[1 + len(sent)]))
            sent[-1].start()
    saved.wait()
    for copy in sent:
        copy.wait()


def call(body, outs, scratch=(), sems=0, cost=1 << 20, ins=pltpu.VMEM, to=pltpu.VMEM, limit=LIMIT):
    def run(*args):
        return pl.pallas_call(
            body,
            out_shape=[jax.ShapeDtypeStruct(s, F32) if isinstance(s, tuple) else s for s in outs],
            in_specs=[pl.BlockSpec(memory_space=ins)] * len(args),
            out_specs=[pl.BlockSpec(memory_space=to)] * len(outs),
            scratch_shapes=[s if not isinstance(s, tuple) else pltpu.VMEM(s, F32) for s in scratch]
            + ([pltpu.SemaphoreType.DMA((sems,))] if sems else []),
            compiler_params=pltpu.CompilerParams(vmem_limit_bytes=limit),
            cost_estimate=pl.CostEstimate(flops=cost, bytes_accessed=cost, transcendentals=0),
        )(*args)

    return run


def pairs(n, k):
    return [(i, i ^ k) for i in range(n)]


def named(send, n):
    out = []
    for k in range(1, n):
        out.append(send(k))
    return out


def shards(n_liq, n_dur, value, utility, liq_rates, dur_rates, upwind, income_rates):
    rows, cols, width = value.shape
    cube, turned, flat, edge = (rows, cols, width), (cols, rows, width), (rows * cols, width), (cols, EDGE, width)
    across_dur, across_liq = turned_shape(cols, rows, width), turned_shape(rows, cols, width)
    across_edge = turned_shape(cols, EDGE, width)
    swap_liq = lambda x, k: lax.ppermute(x, "liq", pairs(n_liq, k))
    swap_dur = lambda x, k: lax.ppermute(x, "dur", pairs(n_dur, k))
    n_chips = n_liq // 2
    l_inv, l_low, l_before, l_beta, l_gamma, own, liq_ups, liq_lows, far = call(
        functools.partial(open_liq, n_liq),
        [cube] * 5 + [(6, cols, width)] + [cube] * 2 + [(2, cols, width)],
        [(2, *cube), (2, 2, cols, width), pltpu.VMEM(cube, jnp.int32)],
        sems=4,
        ins=pltpu.HBM,
        limit=OPEN_LIMIT,
    )(liq_rates, dur_rates, upwind)
    alpha, mine, high, less = call(
        open_source, [cube, (8, cols, width)] + [jax.ShapeDtypeStruct((width, width), BF16)] * 2, [flat]
    )(value, utility, income_rates, own, l_inv, l_low, l_before)
    d_inv, d_low, d_before, d_beta, d_gamma, d_mine, dur_ups, dur_lows = call(
        functools.partial(open_dur, n_dur), [turned] * 5 + [(4, rows, width)] + [across_dur] * 2
    )(dur_rates, upwind)
    between = [(i, i + 1) for i in range(1, n_liq - 1, 2)]
    own_coef = other_coef = chip_coefs = None
    for step in range(STEPS):
        final = step == STEPS - 1
        other = swap_liq(mine, 1)
        if step == 0:
            own_coef, other_coef = mine, other
            joint, half = call(join_core, [(6, cols, width), (6, cols // 2, width)])(mine, other, own_coef, other_coef)
            mine_of = named(lambda k: swap_liq(half, 2 * k), n_chips)
            if n_dur == QUAD:
                its = swap_dur(d_mine, 1)
                (weights,) = call(pair_weights, [(3, rows, width)])(d_mine, its)
                weights = swap_dur(weights, 2)
                d_coefs = [d_mine, its, weights]
            else:
                d_coefs = [d_mine] + [swap_dur(d_mine, k) for k in range(1, n_dur)]
            its_of = named(lambda k: swap_liq(mine_of[k - 1], 1), n_chips)
            chips = [joint, *call(mend, [(6, cols, width)] * (n_chips - 1))(*mine_of, *its_of)]
            chip_coefs = chips
        else:
            (joint,) = call(join_core, [(2, cols, width)])(mine, other, own_coef, other_coef)
            chips = [joint] + named(lambda k: swap_liq(joint, 2 * k), n_chips)
        if final:
            *e_lines, e_beta, e_gamma, e_coef = call(
                functools.partial(open_edge, n_dur), [edge] * 5 + [(EDGE, width)], [across_edge] * 2
            )(other_near, far)
        d_alpha, d_rhs, *e_alpha = call(
            functools.partial(liq_to_dur, n_chips),
            [turned, (2 * rows + 2 * EDGE, width), edge] if final else [turned, (2 * rows, width)],
            [across_dur] + [across_edge] * final,
        )(
            mine, other, own_coef, other_coef, *chips, *chip_coefs, alpha, l_beta, l_gamma, d_inv, d_low, d_before,
            *((*e_lines, e_coef) if final else ()),
        )
        parts = [d_rhs] + named(lambda k: swap_dur(d_rhs, k), n_dur)
        if step == 0:
            other_near = other
            far = lax.ppermute(far, "liq", between + [(j, i) for i, j in between])
        if not final:
            alpha, mine = call(functools.partial(dur_to_liq, n_dur), [cube, (2, cols, width)], [across_liq, flat])(
                *parts, *d_coefs, d_alpha, d_beta, d_gamma, utility, high, less, l_inv, l_low, l_before
            )
    return call(
        functools.partial(close, n_liq, n_dur),
        [cube, cube],
        [turned_shape(rows + 2, cols, width), across_liq, cube, cube],
        sems=5,
        to=pltpu.HBM,
    )(
        *parts, *d_coefs, d_alpha, d_beta, d_gamma, *e_alpha, e_beta, e_gamma,
        utility, high, less, liq_ups, liq_lows, dur_ups, dur_lows,
    )


def solution(mesh):
    n_liq, n_dur = mesh.shape["liq"], mesh.shape["dur"]
    cell = P("liq", "dur", None)
    pair = P(None, "liq", "dur", None)

    def body(*args):
        return shards(n_liq, n_dur, *args)

    return jax.shard_map(
        body,
        mesh=mesh,
        in_specs=(cell, cell, pair, pair, cell, P()),
        out_specs=(cell, cell),
        check_vma=False,
    )
```

```python
import functools

import jax
import jax.numpy as jnp
from jax import lax
from jax.experimental import pallas as pl
from jax.experimental.pallas import tpu as pltpu
from jax.sharding import PartitionSpec as P


STEPS = 2
DISC = 0.05
F32 = jnp.float32
BF16 = jnp.bfloat16
LIMIT = 24 * 1024 * 1024
OPEN_LIMIT = 50 * 1024 * 1024


def meet(left, right):
    a1, a2, b1, c1, b2, c2 = left
    d1, d2, e1, f1, e2, f2 = right
    m = 1.0 / (1.0 - c2 * e1)
    first = (m * (d1 + e1 * a2), m * e1 * b2, m * f1)
    last = (m * (a2 + c2 * d1), m * b2, m * c2 * f1)
    joint = (
        a1 + c1 * first[0],
        d2 + e2 * last[0],
        b1 + c1 * first[1],
        c1 * first[2],
        e2 * last[1],
        f2 + e2 * last[2],
    )
    return first, last, joint


def ordered(swap, own, other):
    left = tuple(jnp.where(swap, o, w) for w, o in zip(own, other))
    right = tuple(jnp.where(swap, w, o) for w, o in zip(own, other))
    return left, right


def descend(place, groups, depth=0):
    if len(groups) == 1:
        return None, None
    swap = ((place >> depth) & 1) == 1
    joints, ours = [], None
    for k in range(0, len(groups), 2):
        left, right = ordered(swap, groups[k], groups[k + 1])
        first, last, joint = meet(left, right)
        ours = ours or (first, last)
        joints.append(joint)
    p, q = descend(place, joints, depth + 1)
    return inside(swap, ours, p, q)


def inside(swap, ours, p, q):
    first, last = ours
    f, l = first[0], last[0]
    if p is not None:
        f = f + first[1] * p + first[2] * q
        l = l + last[1] * p + last[2] * q
    else:
        p, q = jnp.zeros_like(f), jnp.zeros_like(f)
    return jnp.where(swap, l, p), jnp.where(swap, q, f)


def relation(rhs, coef, at):
    part = pl.ds(0, rhs.shape[1])
    return (rhs[0], rhs[1], *(coef[k, part] for k in range(at, at + 4)))


def split(x):
    high = x.astype(BF16)
    return high, (x - high.astype(F32)).astype(BF16)


def income(field, high, low):
    dims = (((1,), (1,)), ((), ()))
    fh, fl = split(field)
    rh, rl = high[...], low[...]
    dot = functools.partial(lax.dot_general, dimension_numbers=dims, preferred_element_type=F32)
    return dot(fh, rh) + (dot(fh, rl) + dot(fl, rh))


def take_rhs(rows, source, inv, low, before, alpha):
    head, prev = None, None
    for k in range(rows):
        now = source(k)
        part = pl.ds(0, now.shape[0])
        now = now * inv[k, part]
        if k:
            now = now + low[k, part] * prev
        alpha[k] = now
        head = now if head is None else head + before[k, part] * now
        prev = now
    return head, prev


def take_matrix(rows, coefs, diag, inv, low, before, beta, gamma):
    b1 = q = bp = gp = None
    for k in range(rows):
        up, lo = coefs(k)
        pivot = diag + up + lo
        if k:
            pivot = pivot - lo * bp
        ip = 1.0 / pivot
        lp = lo * ip
        bp = up * ip
        gp = lp * gp if k else lp
        inv[k] = ip
        low[k] = lp
        beta[k] = bp
        gamma[k] = gp
        before[k] = q if k else jnp.ones_like(ip)
        b1 = b1 + q * gp if k else gp
        q = q * bp if k else bp
    return b1, q, gp, bp


def back(rows, alpha, beta, gamma, p, q, put):
    x = q
    part = pl.ds(0, x.shape[0])
    for k in reversed(range(rows)):
        x = alpha[k] + beta[k, part] * x + gamma[k, part] * p
        put(k, x)


def pick(on, x):
    return jnp.where(on, x, 0.0)


LANES = 128


def stride_of(rows):
    return rows if rows % 16 else rows + 8


def turned_shape(slabs, rows, width):
    return (width // LANES, slabs * stride_of(rows), LANES)


def put_across(turned, k, slabs, rows, x, first=0):
    stride = stride_of(rows)
    for h in range(turned.shape[0]):
        turned[h, pl.ds(first * stride + k, slabs, stride=stride), :] = x[:, h * LANES : (h + 1) * LANES]


def get_slab(turned, slab, rows):
    parts = [turned[h, pl.ds(slab * stride_of(rows), rows), :] for h in range(turned.shape[0])]
    return jnp.concatenate(parts, axis=1)


def fetch(pairs, sems):
    copies = [pltpu.make_async_copy(src, dst, sems.at[k]) for k, (src, dst) in enumerate(pairs)]
    for copy in copies:
        copy.start()
    return copies


def open_liq(n_liq, rates_h, dur_rates_h, upwind_h, *refs):
    inv, low, before, beta, gamma, out, ups, lows, far = refs[:9]
    rates, edges, upwind, sems = refs[9:]
    rows = upwind.shape[0]
    copies = fetch(
        [
            (rates_h, rates),
            (upwind_h, upwind),
            (dur_rates_h.at[:, 0], edges.at[0]),
            (dur_rates_h.at[:, rows - 1], edges.at[1]),
        ],
        sems,
    )
    place = lax.axis_index("liq")

    def coefs(k):
        code = upwind[k]
        up = pick((code & 1) > 0, rates[0, k])
        lo = pick((code & 2) > 0, rates[1, k])
        if k == rows - 1:
            up = pick(place < n_liq - 1, up)
        if k == 0:
            lo = pick(place > 0, lo)
        ups[k], lows[k] = up, lo
        return up, lo

    for copy in copies:
        copy.wait()
    out[0], out[1], out[2], out[3] = take_matrix(rows, coefs, 1.0, inv, low, before, beta, gamma)
    odd = (place & 1) == 1
    for k in range(2):
        head = pick((upwind[0] & (4 << k)) > 0, edges[0, k])
        tail = pick((upwind[rows - 1] & (4 << k)) > 0, edges[1, k])
        out[4 + k] = jnp.where(odd, head, tail)
        far[k] = jnp.where(odd, tail, head)


def open_source(value, utility, income_rates, coef, inv, low, before, alpha, out, high, less, source):
    rows, cols, width = value.shape
    v = value[...].reshape(rows * cols, width)
    high[...], less[...] = split(income_rates[...])
    source[...] = v + income(v, high, less) + utility[...].reshape(v.shape)
    out[0], out[1] = take_rhs(rows, lambda k: source[pl.ds(k * cols, cols), :], inv, low, before, alpha)
    for k in range(coef.shape[0]):
        out[2 + k] = coef[k]


def open_dur(n_dur, rates, upwind, inv, low, before, beta, gamma, out, ups, lows):
    rows, cols = rates.shape[1], rates.shape[2]
    for j, turned in enumerate((ups, lows)):
        for k in range(rows):
            put_across(turned, k, cols, rows, pick((upwind[k] & (4 << j)) > 0, rates[j, k]))
    coefs = dur_coefs(n_dur, cols, rows, ups, lows)
    out[0], out[1], out[2], out[3] = take_matrix(cols, coefs, 1.0 + DISC, inv, low, before, beta, gamma)


def dur_coefs(n_dur, cols, rows, ups, lows):
    place = lax.axis_index("dur")

    def coefs(b):
        up, lo = get_slab(ups, b, rows), get_slab(lows, b, rows)
        if b == cols - 1:
            up = pick(place < n_dur - 1, up)
        if b == 0:
            lo = pick(place > 0, lo)
        return up, lo

    return coefs


EDGE = 8


def put_edges(turned, cols, previous, following):
    put_across(turned, 0, cols, EDGE, previous)
    put_across(turned, 1, cols, EDGE, following)
    for k in range(2, EDGE):
        put_across(turned, k, cols, EDGE, jnp.zeros_like(previous))


def open_edge(n_dur, near, far, inv, low, before, beta, gamma, out, ups, lows):
    odd = (lax.axis_index("liq") & 1) == 1
    cols = inv.shape[0]
    for j, turned in enumerate((ups, lows)):
        put_edges(turned, cols, jnp.where(odd, near[6 + j], far[j]), jnp.where(odd, far[j], near[6 + j]))
    coefs = dur_coefs(n_dur, cols, EDGE, ups, lows)
    matrix = take_matrix(cols, coefs, 1.0 + DISC, inv, low, before, beta, gamma)
    out[...] = jnp.concatenate([m[:2] for m in matrix], axis=0)


def join_share(own, other, own_coef, other_coef, share, out, sent):
    join_core(own, other, own_coef, other_coef, out)
    sent[0] = share[0] * out[0] + share[1] * out[1]


def join_core(own, other, own_coef, other_coef, out, *half):
    swap = (lax.axis_index("liq") & 1) == 1
    left, right = ordered(swap, relation(own, own_coef, 2), relation(other, other_coef, 2))
    joint = meet(left, right)[2]
    for k in range(out.shape[0]):
        out[k] = joint[k]
    for part in half:
        lines = part.shape[1]
        for k in range(out.shape[0]):
            part[k] = jnp.where(swap, joint[k][lines:], joint[k][:lines])


def mend(n, joint, *refs):
    place = lax.axis_index("liq")
    swap = (place & 1) == 1
    outs = refs[2 * n :]
    for mine, other, out in zip(refs[:n], refs[n : 2 * n], outs):
        lines = mine.shape[1]
        for k in range(out.shape[0]):
            out[k, pl.ds(0, lines)] = jnp.where(swap, other[k], mine[k])
            out[k, pl.ds(lines, lines)] = jnp.where(swap, mine[k], other[k])
    if n + 1 == QUAD:
        slope, share = outs[n:]
        chip = place >> 1
        swap, upper = sides(chip)
        own, its, one, two = (tuple(ref[2 + k] for k in range(4)) for ref in (joint, *outs[:n]))
        slope[...] = joint_slope(~upper, *ordered(swap, one, two))
        share[0], share[1] = shares(chip, own, its)


def liq_to_dur(n_chips, n_coefs, quad, final, *refs):
    refs = list(refs)

    def take(n):
        taken = refs[:n]
        del refs[:n]
        return taken

    own, other, own_coef, other_coef = take(4)
    chips, chip_coefs = take(n_chips), take(n_coefs)
    alpha, beta, gamma, inv, low, before = take(6)
    share = take(quad)
    if final:
        e_inv, e_low, e_before, e_coef = take(4)
    alpha_out, *outs = take(2 + quad)
    if final:
        (e_alpha,) = take(1)
    turned = refs[0]
    swap = (lax.axis_index("liq") & 1) == 1
    left, right = ordered(swap, relation(own, own_coef, 2), relation(other, other_coef, 2))
    first, last, _ = meet(left, right)
    p, q = beside_chips(chips, chip_coefs)
    p, q = inside(swap, (first, last), p, q)
    rows, cols = alpha.shape[0], alpha.shape[1]
    if final:
        e_turned = refs[1]
        put_edges(e_turned, cols, p, q)
        ends = take_rhs(cols, lambda b: get_slab(e_turned, b, EDGE), e_inv, e_low, e_before, e_alpha)
        ends = jnp.concatenate([e[:2] for e in ends + ends], axis=0)
        for out in outs:
            out[pl.ds(out.shape[0] - 2 * EDGE, EDGE)] = ends
            out[pl.ds(out.shape[0] - EDGE, EDGE)] = e_coef[...]
    back(rows, alpha, beta, gamma, p, q, lambda k, x: put_across(turned, k, cols, rows, x))
    ends = take_rhs(cols, lambda b: get_slab(turned, b, rows), inv, low, before, alpha_out)
    for k in range(2):
        outs[0][pl.ds(k * rows, rows)] = ends[k]
    if quad:
        outs[1][pl.ds(0, rows)] = share[0][0] * ends[0] + share[0][1] * ends[1]


QUAD = 4


def sides(place):
    return (place & 1) == 1, (place & 2) == 2


def joint_slope(upper, left, right):
    (b1, c1, b2, c2), (e1, f1, e2, f2) = left, right
    m = 1.0 / (1.0 - c2 * e1)
    return jnp.where(upper, b1 + c1 * m * e1 * b2, f2 + e2 * m * c2 * f1)


def shares(place, own, its):
    swap, upper = sides(place)
    (b1, c1, b2, c2), (e1, f1, e2, f2) = ordered(swap, own, its)
    m = 1.0 / (1.0 - c2 * e1)
    one, none = jnp.ones_like(m), jnp.zeros_like(m)
    first = jnp.where(upper, jnp.where(swap, c1 * m, one), jnp.where(swap, e2 * m * c2, none))
    second = jnp.where(upper, jnp.where(swap, none, c1 * m * e1), jnp.where(swap, one, e2 * m))
    return first, second


def beside_pair(place, own, its, far, far_slope):
    swap, upper = sides(place)
    first, last, joint = meet(*ordered(swap, own, its))
    ours = jnp.where(upper, joint[0], joint[1])
    slope = jnp.where(upper, joint[2], joint[5])
    beyond = (far + far_slope * ours) / (1.0 - far_slope * slope)
    none = jnp.zeros_like(beyond)
    return inside(swap, (first, last), jnp.where(upper, beyond, none), jnp.where(upper, none, beyond))


def pair_weights(own, other, slope, share):
    place = lax.axis_index("dur")
    swap, upper = sides(place)
    mine, its = (tuple(ref[k] for k in range(4)) for ref in (own, other))
    slope[...] = joint_slope(upper, *ordered(swap, mine, its))
    share[0], share[1] = shares(place, mine, its)


def beside_dur(parts, coefs):
    place = lax.axis_index("dur")
    rows = coefs[0].shape[1]
    known = [
        tuple(ref[pl.ds(k * rows, rows)] for k in range(2)) + tuple(c[k] for k in range(4))
        for ref, c in zip(parts, coefs[:2] if len(parts) == QUAD else coefs)
    ]
    if len(parts) != QUAD:
        return descend(place, known)
    part = pl.ds(0, rows)
    return beside_pair(place, *known, parts[2][part] + parts[3][part], coefs[2][...])


def beside_chips(chips, coefs):
    place = lax.axis_index("liq") >> 1
    if len(coefs) == len(chips):
        return descend(place, [relation(r, c, 2) for r, c in zip(chips, coefs)])
    own, its = (relation(r, c, 2) for r, c in zip(chips[:2], coefs[:2]))
    return beside_pair(place, own, its, chips[2][0] + chips[3][0], coefs[2][...])


def beside_edge(parts):
    def piece(ref, k):
        return ref[pl.ds(k, 2)]

    def known(ref):
        start = ref.shape[0] - 2 * EDGE
        return tuple(piece(ref, start + k) for k in [0, 2] + [EDGE + 2 * k for k in range(4)])

    return descend(lax.axis_index("dur"), [known(ref) for ref in parts])


def given_dur(n_dur, refs):
    coefs = 3 if n_dur == QUAD else n_dur
    return refs[:n_dur], refs[n_dur : n_dur + coefs], refs[n_dur + coefs :]


def dur_to_liq(n_dur, *refs):
    parts, coefs, refs = given_dur(n_dur, refs)
    alpha, beta, gamma, utility, high, less, inv, low, before, alpha_out, out, field, source = refs
    p, q = beside_dur(parts, coefs)
    rows, cols = utility.shape[0], utility.shape[1]
    back(cols, alpha, beta, gamma, p, q, lambda b, x: put_across(field, b, rows, cols, x))
    v = jnp.concatenate([get_slab(field, k, cols) for k in range(rows)], axis=0)
    source[...] = v + income(v, high, less) + utility[...].reshape(v.shape)
    out[0], out[1] = take_rhs(rows, lambda k: source[pl.ds(k * cols, cols), :], inv, low, before, alpha_out)


def close(n_liq, n_dur, *refs):
    parts, coefs, refs = given_dur(n_dur, refs)
    alpha, beta, gamma, e_alpha, e_beta, e_gamma = refs[:6]
    utility, high, less, liq_ups, liq_lows, dur_ups, dur_lows = refs[6:13]
    value_h, out_h, field, drift, value, out, sems = refs[13:]
    rows, cols, width = utility.shape
    liq, dur = lax.axis_index("liq"), lax.axis_index("dur")
    p, q = beside_dur(parts, coefs)
    after, here = jnp.where(dur < n_dur - 1, q, 0.0), None
    x = q
    rates = dur_coefs(n_dur, cols, rows, dur_ups, dur_lows)

    def flow(b, here, after, ahead):
        up, lo = rates(b)
        put_across(drift, b, rows, cols, up * (after - here) + lo * (ahead - here))

    for b in reversed(range(cols)):
        x = alpha[b] + beta[b] * x + gamma[b] * p
        put_across(field, b, rows, cols, x)
        if here is not None:
            flow(b + 1, here, after, x)
            after = here
        here = x
    flow(0, here, after, p)
    p, x = beside_edge(parts)
    for b in reversed(range(cols)):
        x = e_alpha[b, :2] + e_beta[b, :2] * x + e_gamma[b, :2] * p
        put_across(field, b, 2, cols, x, first=rows)
    for k in range(rows):
        value[k] = get_slab(field, k, cols)
    saved = pltpu.make_async_copy(value, value_h, sems.at[0])
    saved.start()
    v = value[...].reshape(rows * cols, width)
    out[...] = (income(v, high, less) - DISC * v).reshape(out.shape) + utility[...]
    parts = 4
    sent = []
    for k in range(rows):
        here = value[k]
        up = value[k + 1] if k < rows - 1 else jnp.where(liq < n_liq - 1, get_slab(field, rows + 1, cols), here)
        lo = value[k - 1] if k else jnp.where(liq > 0, get_slab(field, rows, cols), here)
        moved = liq_ups[k] * (up - here) + liq_lows[k] * (lo - here) + get_slab(drift, k, cols)
        out[k] = out[k] + moved
        if (k + 1) % (rows // parts) == 0:
            piece = pl.ds(k + 1 - rows // parts, rows // parts)
            sent.append(pltpu.make_async_copy(out.at[piece], out_h.at[piece], sems.at[1 + len(sent)]))
            sent[-1].start()
    saved.wait()
    for copy in sent:
        copy.wait()


def call(body, outs, scratch=(), sems=0, cost=1 << 20, ins=pltpu.VMEM, to=pltpu.VMEM, limit=LIMIT):
    def run(*args):
        return pl.pallas_call(
            body,
            out_shape=[jax.ShapeDtypeStruct(s, F32) if isinstance(s, tuple) else s for s in outs],
            in_specs=[pl.BlockSpec(memory_space=ins)] * len(args),
            out_specs=[pl.BlockSpec(memory_space=to)] * len(outs),
            scratch_shapes=[s if not isinstance(s, tuple) else pltpu.VMEM(s, F32) for s in scratch]
            + ([pltpu.SemaphoreType.DMA((sems,))] if sems else []),
            compiler_params=pltpu.CompilerParams(vmem_limit_bytes=limit),
            cost_estimate=pl.CostEstimate(flops=cost, bytes_accessed=cost, transcendentals=0),
        )(*args)

    return run


def pairs(n, k):
    return [(i, i ^ k) for i in range(n)]


def named(send, n):
    out = []
    for k in range(1, n):
        out.append(send(k))
    return out


def shards(n_liq, n_dur, value, utility, liq_rates, dur_rates, upwind, income_rates):
    rows, cols, width = value.shape
    cube, turned, flat, edge = (rows, cols, width), (cols, rows, width), (rows * cols, width), (cols, EDGE, width)
    across_dur, across_liq = turned_shape(cols, rows, width), turned_shape(rows, cols, width)
    across_edge = turned_shape(cols, EDGE, width)
    swap_liq = lambda x, k: lax.ppermute(x, "liq", pairs(n_liq, k))
    swap_dur = lambda x, k: lax.ppermute(x, "dur", pairs(n_dur, k))
    n_chips = n_liq // 2
    l_inv, l_low, l_before, l_beta, l_gamma, own, liq_ups, liq_lows, far = call(
        functools.partial(open_liq, n_liq),
        [cube] * 5 + [(6, cols, width)] + [cube] * 2 + [(2, cols, width)],
        [(2, *cube), (2, 2, cols, width), pltpu.VMEM(cube, jnp.int32)],
        sems=4,
        ins=pltpu.HBM,
        limit=OPEN_LIMIT,
    )(liq_rates, dur_rates, upwind)
    alpha, mine, high, less = call(
        open_source, [cube, (8, cols, width)] + [jax.ShapeDtypeStruct((width, width), BF16)] * 2, [flat]
    )(value, utility, income_rates, own, l_inv, l_low, l_before)
    d_inv, d_low, d_before, d_beta, d_gamma, d_mine, dur_ups, dur_lows = call(
        functools.partial(open_dur, n_dur), [turned] * 5 + [(4, rows, width)] + [across_dur] * 2
    )(dur_rates, upwind)
    between = [(i, i + 1) for i in range(1, n_liq - 1, 2)]
    own_coef = other_coef = chip_coefs = None
    for step in range(STEPS):
        final = step == STEPS - 1
        other = swap_liq(mine, 1)
        if step == 0:
            own_coef, other_coef = mine, other
            joint, half = call(join_core, [(6, cols, width), (6, cols // 2, width)])(mine, other, own_coef, other_coef)
            mine_of = named(lambda k: swap_liq(half, 2 * k), n_chips)
            if n_dur == QUAD:
                its = swap_dur(d_mine, 1)
                slope, *d_share = call(pair_weights, [(rows, width), (2, rows, width)])(d_mine, its)
                slope = swap_dur(slope, 2)
                d_coefs = [d_mine, its, slope]
            else:
                d_coefs = [d_mine] + [swap_dur(d_mine, k) for k in range(1, n_dur)]
            its_of = named(lambda k: swap_liq(mine_of[k - 1], 1), n_chips)
            more = [(cols, width), (2, cols, width)] if n_chips == QUAD else []
            mended = call(functools.partial(mend, n_chips - 1), [(6, cols, width)] * (n_chips - 1) + more)(
                joint, *mine_of, *its_of
            )
            chips = [joint, *mended[: n_chips - 1]]
            chip_coefs = chips
        elif n_chips == QUAD:
            joint, sent = call(join_share, [(2, cols, width), (1, cols, width)])(
                mine, other, own_coef, other_coef, mended[-1]
            )
            chips = [joint] + named(lambda k: swap_liq(joint if k == 1 else sent, 2 * k), n_chips)
            chip_coefs = [*chip_coefs[:2], mended[-2]]
        else:
            (joint,) = call(join_core, [(2, cols, width)])(mine, other, own_coef, other_coef)
            chips = [joint] + named(lambda k: swap_liq(joint, 2 * k), n_chips)
        if final:
            *e_lines, e_beta, e_gamma, e_coef = call(
                functools.partial(open_edge, n_dur), [edge] * 5 + [(EDGE, width)], [across_edge] * 2
            )(other_near, far)
        quad, extra = n_dur == QUAD, 2 * EDGE * final
        d_alpha, *outs = call(
            functools.partial(liq_to_dur, n_chips, len(chip_coefs), quad, final),
            [turned, (2 * rows + extra, width)] + [(rows + extra, width)] * quad + [edge] * final,
            [across_dur] + [across_edge] * final,
        )(
            mine, other, own_coef, other_coef, *chips, *chip_coefs, alpha, l_beta, l_gamma, d_inv, d_low, d_before,
            *(d_share if quad else ()), *((*e_lines, e_coef) if final else ()),
        )
        e_alpha = outs[1 + quad :]
        parts = outs[:1] + named(lambda k: swap_dur(outs[int(quad and k > 1)], k), n_dur)
        if step == 0:
            other_near = other
            far = lax.ppermute(far, "liq", between + [(j, i) for i, j in between])
        if not final:
            alpha, mine = call(functools.partial(dur_to_liq, n_dur), [cube, (2, cols, width)], [across_liq, flat])(
                *parts, *d_coefs, d_alpha, d_beta, d_gamma, utility, high, less, l_inv, l_low, l_before
            )
    return call(
        functools.partial(close, n_liq, n_dur),
        [cube, cube],
        [turned_shape(rows + 2, cols, width), across_liq, cube, cube],
        sems=5,
        to=pltpu.HBM,
    )(
        *parts, *d_coefs, d_alpha, d_beta, d_gamma, *e_alpha, e_beta, e_gamma,
        utility, high, less, liq_ups, liq_lows, dur_ups, dur_lows,
    )


def solution(mesh):
    n_liq, n_dur = mesh.shape["liq"], mesh.shape["dur"]
    cell = P("liq", "dur", None)
    pair = P(None, "liq", "dur", None)

    def body(*args):
        return shards(n_liq, n_dur, *args)

    return jax.shard_map(
        body,
        mesh=mesh,
        in_specs=(cell, cell, pair, pair, cell, P()),
        out_specs=(cell, cell),
        check_vma=False,
    )
```

```python
import functools

import jax
import jax.numpy as jnp
from jax import lax
from jax.experimental import pallas as pl
from jax.experimental.pallas import tpu as pltpu
from jax.sharding import PartitionSpec as P


STEPS = 2
DISC = 0.05
F32 = jnp.float32
BF16 = jnp.bfloat16
LIMIT = 24 * 1024 * 1024
OPEN_LIMIT = 50 * 1024 * 1024


def meet(left, right):
    a1, a2, b1, c1, b2, c2 = left
    d1, d2, e1, f1, e2, f2 = right
    m = 1.0 / (1.0 - c2 * e1)
    first = (m * (d1 + e1 * a2), m * e1 * b2, m * f1)
    last = (m * (a2 + c2 * d1), m * b2, m * c2 * f1)
    joint = (
        a1 + c1 * first[0],
        d2 + e2 * last[0],
        b1 + c1 * first[1],
        c1 * first[2],
        e2 * last[1],
        f2 + e2 * last[2],
    )
    return first, last, joint


def ordered(swap, own, other):
    left = tuple(jnp.where(swap, o, w) for w, o in zip(own, other))
    right = tuple(jnp.where(swap, w, o) for w, o in zip(own, other))
    return left, right


def descend(place, groups, depth=0):
    if len(groups) == 1:
        return None, None
    swap = ((place >> depth) & 1) == 1
    joints, ours = [], None
    for k in range(0, len(groups), 2):
        left, right = ordered(swap, groups[k], groups[k + 1])
        first, last, joint = meet(left, right)
        ours = ours or (first, last)
        joints.append(joint)
    p, q = descend(place, joints, depth + 1)
    return inside(swap, ours, p, q)


def inside(swap, ours, p, q):
    first, last = ours
    f, l = first[0], last[0]
    if p is not None:
        f = f + first[1] * p + first[2] * q
        l = l + last[1] * p + last[2] * q
    else:
        p, q = jnp.zeros_like(f), jnp.zeros_like(f)
    return jnp.where(swap, l, p), jnp.where(swap, q, f)


def relation(rhs, coef, at):
    part = pl.ds(0, rhs.shape[1])
    return (rhs[0], rhs[1], *(coef[k, part] for k in range(at, at + 4)))


def split(x):
    high = x.astype(BF16)
    return high, (x - high.astype(F32)).astype(BF16)


def income(field, high, low):
    dims = (((1,), (1,)), ((), ()))
    fh, fl = split(field)
    rh, rl = high[...], low[...]
    dot = functools.partial(lax.dot_general, dimension_numbers=dims, preferred_element_type=F32)
    return dot(fh, rh) + (dot(fh, rl) + dot(fl, rh))


def take_rhs(rows, source, inv, low, before, alpha):
    head, prev = None, None
    for k in range(rows):
        now = source(k)
        part = pl.ds(0, now.shape[0])
        now = now * inv[k, part]
        if k:
            now = now + low[k, part] * prev
        alpha[k] = now
        head = now if head is None else head + before[k, part] * now
        prev = now
    return head, prev


def take_matrix(rows, coefs, diag, inv, low, before, beta, gamma):
    b1 = q = bp = gp = None
    for k in range(rows):
        up, lo = coefs(k)
        pivot = diag + up + lo
        if k:
            pivot = pivot - lo * bp
        ip = 1.0 / pivot
        lp = lo * ip
        bp = up * ip
        gp = lp * gp if k else lp
        inv[k] = ip
        low[k] = lp
        beta[k] = bp
        gamma[k] = gp
        before[k] = q if k else jnp.ones_like(ip)
        b1 = b1 + q * gp if k else gp
        q = q * bp if k else bp
    return b1, q, gp, bp


def back(rows, alpha, beta, gamma, p, q, put):
    x = q
    part = pl.ds(0, x.shape[0])
    for k in reversed(range(rows)):
        x = alpha[k] + beta[k, part] * x + gamma[k, part] * p
        put(k, x)


def pick(on, x):
    return jnp.where(on, x, 0.0)


LANES = 128


def stride_of(rows):
    return rows + 1


def turned_shape(slabs, rows, width):
    return (width // LANES, -(-slabs * stride_of(rows) // 8) * 8, LANES)


def put_across(turned, k, slabs, rows, x, first=0):
    stride = stride_of(rows)
    for h in range(turned.shape[0]):
        turned[h, pl.ds(first * stride + k, slabs, stride=stride), :] = x[:, h * LANES : (h + 1) * LANES]


def get_slab(turned, slab, rows):
    parts = [turned[h, pl.ds(slab * stride_of(rows), rows), :] for h in range(turned.shape[0])]
    return jnp.concatenate(parts, axis=1)


CHUNKS = 4


def fetch(pairs, sems):
    copies = [pltpu.make_async_copy(src, dst, sems.at[k]) for k, (src, dst) in enumerate(pairs)]
    for copy in copies:
        copy.start()
    return copies


def open_liq(n_liq, rates_h, dur_rates_h, upwind_h, *refs):
    inv, low, before, beta, gamma, out, ups, lows, far = refs[:9]
    rates, edges, upwind, sems = refs[9:]
    rows = upwind.shape[0]
    chunk = rows // CHUNKS
    pieces = [pl.ds(k * chunk, chunk) for k in range(CHUNKS)]
    parts = [(upwind_h.at[p], upwind.at[p]) for p in pieces]
    parts += [(rates_h.at[:, p], rates.at[:, p]) for p in pieces]
    parts = [part for pair in zip(parts[:CHUNKS], parts[CHUNKS:]) for part in pair]
    parts += [(dur_rates_h.at[:, k], edges.at[j]) for j, k in enumerate((0, rows - 1))]
    copies = fetch(parts, sems)
    place = lax.axis_index("liq")

    def coefs(k):
        if k % chunk == 0:
            for copy in copies[2 * (k // chunk) : 2 * (k // chunk) + 2]:
                copy.wait()
        code = upwind[k]
        up = pick((code & 1) > 0, rates[0, k])
        lo = pick((code & 2) > 0, rates[1, k])
        if k == rows - 1:
            up = pick(place < n_liq - 1, up)
        if k == 0:
            lo = pick(place > 0, lo)
        ups[k], lows[k] = up, lo
        return up, lo

    out[0], out[1], out[2], out[3] = take_matrix(rows, coefs, 1.0, inv, low, before, beta, gamma)
    for copy in copies[2 * CHUNKS :]:
        copy.wait()
    odd = (place & 1) == 1
    for k in range(2):
        head = pick((upwind[0] & (4 << k)) > 0, edges[0, k])
        tail = pick((upwind[rows - 1] & (4 << k)) > 0, edges[1, k])
        out[4 + k] = jnp.where(odd, head, tail)
        far[k] = jnp.where(odd, tail, head)


def open_source(value, utility, income_rates, coef, inv, low, before, alpha, out, high, less, source):
    rows, cols, width = value.shape
    v = value[...].reshape(rows * cols, width)
    high[...], less[...] = split(income_rates[...])
    source[...] = v + income(v, high, less) + utility[...].reshape(v.shape)
    out[0], out[1] = take_rhs(rows, lambda k: source[pl.ds(k * cols, cols), :], inv, low, before, alpha)
    for k in range(coef.shape[0]):
        out[2 + k] = coef[k]


def open_dur(n_dur, rates, upwind, inv, low, before, beta, gamma, out, ups, lows):
    rows, cols = rates.shape[1], rates.shape[2]
    for j, turned in enumerate((ups, lows)):
        for k in range(rows):
            put_across(turned, k, cols, rows, pick((upwind[k] & (4 << j)) > 0, rates[j, k]))
    coefs = dur_coefs(n_dur, cols, rows, ups, lows)
    out[0], out[1], out[2], out[3] = take_matrix(cols, coefs, 1.0 + DISC, inv, low, before, beta, gamma)


def dur_coefs(n_dur, cols, rows, ups, lows):
    place = lax.axis_index("dur")

    def coefs(b):
        up, lo = get_slab(ups, b, rows), get_slab(lows, b, rows)
        if b == cols - 1:
            up = pick(place < n_dur - 1, up)
        if b == 0:
            lo = pick(place > 0, lo)
        return up, lo

    return coefs


EDGE = 8


def put_edges(turned, cols, previous, following):
    put_across(turned, 0, cols, EDGE, previous)
    put_across(turned, 1, cols, EDGE, following)
    for k in range(2, EDGE):
        put_across(turned, k, cols, EDGE, jnp.zeros_like(previous))


def open_edge(n_dur, near, far, inv, low, before, beta, gamma, out, ups, lows):
    odd = (lax.axis_index("liq") & 1) == 1
    cols = inv.shape[0]
    for j, turned in enumerate((ups, lows)):
        put_edges(turned, cols, jnp.where(odd, near[6 + j], far[j]), jnp.where(odd, far[j], near[6 + j]))
    coefs = dur_coefs(n_dur, cols, EDGE, ups, lows)
    matrix = take_matrix(cols, coefs, 1.0 + DISC, inv, low, before, beta, gamma)
    out[...] = jnp.concatenate([m[:2] for m in matrix], axis=0)


def join_share(own, other, own_coef, other_coef, share, out, sent):
    join_core(own, other, own_coef, other_coef, out)
    sent[0] = share[0] * out[0] + share[1] * out[1]


def join_core(own, other, own_coef, other_coef, out, *half):
    swap = (lax.axis_index("liq") & 1) == 1
    left, right = ordered(swap, relation(own, own_coef, 2), relation(other, other_coef, 2))
    joint = meet(left, right)[2]
    for k in range(out.shape[0]):
        out[k] = joint[k]
    for part in half:
        lines = part.shape[1]
        for k in range(out.shape[0]):
            part[k] = jnp.where(swap, joint[k][lines:], joint[k][:lines])


def mend(n, joint, *refs):
    place = lax.axis_index("liq")
    swap = (place & 1) == 1
    outs = refs[2 * n :]
    for mine, other, out in zip(refs[:n], refs[n : 2 * n], outs):
        lines = mine.shape[1]
        for k in range(out.shape[0]):
            out[k, pl.ds(0, lines)] = jnp.where(swap, other[k], mine[k])
            out[k, pl.ds(lines, lines)] = jnp.where(swap, mine[k], other[k])
    if n + 1 == QUAD:
        slope, share = outs[n:]
        chip = place >> 1
        swap, upper = sides(chip)
        own, its, one, two = (tuple(ref[2 + k] for k in range(4)) for ref in (joint, *outs[:n]))
        slope[...] = joint_slope(~upper, *ordered(swap, one, two))
        share[0], share[1] = shares(chip, own, its)


def liq_to_dur(n_chips, n_coefs, quad, final, *refs):
    refs = list(refs)

    def take(n):
        taken = refs[:n]
        del refs[:n]
        return taken

    own, other, own_coef, other_coef = take(4)
    chips, chip_coefs = take(n_chips), take(n_coefs)
    alpha, beta, gamma, inv, low, before = take(6)
    share = take(quad)
    if final:
        e_inv, e_low, e_before, e_coef = take(4)
    alpha_out, *outs = take(2 + quad)
    if final:
        (e_alpha,) = take(1)
    turned = refs[0]
    swap = (lax.axis_index("liq") & 1) == 1
    left, right = ordered(swap, relation(own, own_coef, 2), relation(other, other_coef, 2))
    first, last, _ = meet(left, right)
    p, q = beside_chips(chips, chip_coefs)
    p, q = inside(swap, (first, last), p, q)
    rows, cols = alpha.shape[0], alpha.shape[1]
    if final:
        e_turned = refs[1]
        put_edges(e_turned, cols, p, q)
        ends = take_rhs(cols, lambda b: get_slab(e_turned, b, EDGE), e_inv, e_low, e_before, e_alpha)
        ends = jnp.concatenate([e[:2] for e in ends + ends], axis=0)
        for out in outs:
            out[pl.ds(out.shape[0] - 2 * EDGE, EDGE)] = ends
            out[pl.ds(out.shape[0] - EDGE, EDGE)] = e_coef[...]
    back(rows, alpha, beta, gamma, p, q, lambda k, x: put_across(turned, k, cols, rows, x))
    ends = take_rhs(cols, lambda b: get_slab(turned, b, rows), inv, low, before, alpha_out)
    for k in range(2):
        outs[0][pl.ds(k * rows, rows)] = ends[k]
    if quad:
        outs[1][pl.ds(0, rows)] = share[0][0] * ends[0] + share[0][1] * ends[1]


QUAD = 4


def sides(place):
    return (place & 1) == 1, (place & 2) == 2


def joint_slope(upper, left, right):
    (b1, c1, b2, c2), (e1, f1, e2, f2) = left, right
    m = 1.0 / (1.0 - c2 * e1)
    return jnp.where(upper, b1 + c1 * m * e1 * b2, f2 + e2 * m * c2 * f1)


def shares(place, own, its):
    swap, upper = sides(place)
    (b1, c1, b2, c2), (e1, f1, e2, f2) = ordered(swap, own, its)
    m = 1.0 / (1.0 - c2 * e1)
    one, none = jnp.ones_like(m), jnp.zeros_like(m)
    first = jnp.where(upper, jnp.where(swap, c1 * m, one), jnp.where(swap, e2 * m * c2, none))
    second = jnp.where(upper, jnp.where(swap, none, c1 * m * e1), jnp.where(swap, one, e2 * m))
    return first, second


def beside_pair(place, own, its, far, far_slope):
    swap, upper = sides(place)
    first, last, joint = meet(*ordered(swap, own, its))
    ours = jnp.where(upper, joint[0], joint[1])
    slope = jnp.where(upper, joint[2], joint[5])
    beyond = (far + far_slope * ours) / (1.0 - far_slope * slope)
    none = jnp.zeros_like(beyond)
    return inside(swap, (first, last), jnp.where(upper, beyond, none), jnp.where(upper, none, beyond))


def pair_weights(own, other, slope, share):
    place = lax.axis_index("dur")
    swap, upper = sides(place)
    mine, its = (tuple(ref[k] for k in range(4)) for ref in (own, other))
    slope[...] = joint_slope(upper, *ordered(swap, mine, its))
    share[0], share[1] = shares(place, mine, its)


def beside_dur(parts, coefs):
    place = lax.axis_index("dur")
    rows = coefs[0].shape[1]
    known = [
        tuple(ref[pl.ds(k * rows, rows)] for k in range(2)) + tuple(c[k] for k in range(4))
        for ref, c in zip(parts, coefs[:2] if len(parts) == QUAD else coefs)
    ]
    if len(parts) != QUAD:
        return descend(place, known)
    part = pl.ds(0, rows)
    return beside_pair(place, *known, parts[2][part] + parts[3][part], coefs[2][...])


def beside_chips(chips, coefs):
    place = lax.axis_index("liq") >> 1
    if len(coefs) == len(chips):
        return descend(place, [relation(r, c, 2) for r, c in zip(chips, coefs)])
    own, its = (relation(r, c, 2) for r, c in zip(chips[:2], coefs[:2]))
    return beside_pair(place, own, its, chips[2][0] + chips[3][0], coefs[2][...])


def beside_edge(parts):
    def piece(ref, k):
        return ref[pl.ds(k, 2)]

    def known(ref):
        start = ref.shape[0] - 2 * EDGE
        return tuple(piece(ref, start + k) for k in [0, 2] + [EDGE + 2 * k for k in range(4)])

    return descend(lax.axis_index("dur"), [known(ref) for ref in parts])


def given_dur(n_dur, refs):
    coefs = 3 if n_dur == QUAD else n_dur
    return refs[:n_dur], refs[n_dur : n_dur + coefs], refs[n_dur + coefs :]


def dur_to_liq(n_dur, *refs):
    parts, coefs, refs = given_dur(n_dur, refs)
    alpha, beta, gamma, utility, high, less, inv, low, before, alpha_out, out, field, source = refs
    p, q = beside_dur(parts, coefs)
    rows, cols = utility.shape[0], utility.shape[1]
    back(cols, alpha, beta, gamma, p, q, lambda b, x: put_across(field, b, rows, cols, x))
    v = jnp.concatenate([get_slab(field, k, cols) for k in range(rows)], axis=0)
    source[...] = v + income(v, high, less) + utility[...].reshape(v.shape)
    out[0], out[1] = take_rhs(rows, lambda k: source[pl.ds(k * cols, cols), :], inv, low, before, alpha_out)


def close(n_liq, n_dur, *refs):
    parts, coefs, refs = given_dur(n_dur, refs)
    alpha, beta, gamma, e_alpha, e_beta, e_gamma = refs[:6]
    utility, high, less, liq_ups, liq_lows, dur_ups, dur_lows = refs[6:13]
    value_h, out_h, field, drift, value, out, sems = refs[13:]
    rows, cols, width = utility.shape
    liq, dur = lax.axis_index("liq"), lax.axis_index("dur")
    p, q = beside_dur(parts, coefs)
    after, here = jnp.where(dur < n_dur - 1, q, 0.0), None
    x = q
    rates = dur_coefs(n_dur, cols, rows, dur_ups, dur_lows)

    def flow(b, here, after, ahead):
        up, lo = rates(b)
        put_across(drift, b, rows, cols, up * (after - here) + lo * (ahead - here))

    for b in reversed(range(cols)):
        x = alpha[b] + beta[b] * x + gamma[b] * p
        put_across(field, b, rows, cols, x)
        if here is not None:
            flow(b + 1, here, after, x)
            after = here
        here = x
    flow(0, here, after, p)
    p, x = beside_edge(parts)
    for b in reversed(range(cols)):
        x = e_alpha[b, :2] + e_beta[b, :2] * x + e_gamma[b, :2] * p
        put_across(field, b, 2, cols, x, first=rows)
    for k in range(rows):
        value[k] = get_slab(field, k, cols)
    saved = pltpu.make_async_copy(value, value_h, sems.at[0])
    saved.start()
    v = value[...].reshape(rows * cols, width)
    out[...] = (income(v, high, less) - DISC * v).reshape(out.shape) + utility[...]
    parts = 4
    sent = []
    for k in range(rows):
        here = value[k]
        up = value[k + 1] if k < rows - 1 else jnp.where(liq < n_liq - 1, get_slab(field, rows + 1, cols), here)
        lo = value[k - 1] if k else jnp.where(liq > 0, get_slab(field, rows, cols), here)
        moved = liq_ups[k] * (up - here) + liq_lows[k] * (lo - here) + get_slab(drift, k, cols)
        out[k] = out[k] + moved
        if (k + 1) % (rows // parts) == 0:
            piece = pl.ds(k + 1 - rows // parts, rows // parts)
            sent.append(pltpu.make_async_copy(out.at[piece], out_h.at[piece], sems.at[1 + len(sent)]))
            sent[-1].start()
    saved.wait()
    for copy in sent:
        copy.wait()


def call(body, outs, scratch=(), sems=0, cost=1 << 20, ins=pltpu.VMEM, to=pltpu.VMEM, limit=LIMIT):
    def run(*args):
        return pl.pallas_call(
            body,
            out_shape=[jax.ShapeDtypeStruct(s, F32) if isinstance(s, tuple) else s for s in outs],
            in_specs=[pl.BlockSpec(memory_space=ins)] * len(args),
            out_specs=[pl.BlockSpec(memory_space=to)] * len(outs),
            scratch_shapes=[s if not isinstance(s, tuple) else pltpu.VMEM(s, F32) for s in scratch]
            + ([pltpu.SemaphoreType.DMA((sems,))] if sems else []),
            compiler_params=pltpu.CompilerParams(vmem_limit_bytes=limit),
            cost_estimate=pl.CostEstimate(flops=cost, bytes_accessed=cost, transcendentals=0),
        )(*args)

    return run


def pairs(n, k):
    return [(i, i ^ k) for i in range(n)]


def named(send, n):
    out = []
    for k in range(1, n):
        out.append(send(k))
    return out


def shards(n_liq, n_dur, value, utility, liq_rates, dur_rates, upwind, income_rates):
    rows, cols, width = value.shape
    cube, turned, flat, edge = (rows, cols, width), (cols, rows, width), (rows * cols, width), (cols, EDGE, width)
    across_dur, across_liq = turned_shape(cols, rows, width), turned_shape(rows, cols, width)
    across_edge = turned_shape(cols, EDGE, width)
    swap_liq = lambda x, k: lax.ppermute(x, "liq", pairs(n_liq, k))
    swap_dur = lambda x, k: lax.ppermute(x, "dur", pairs(n_dur, k))
    n_chips = n_liq // 2
    l_inv, l_low, l_before, l_beta, l_gamma, own, liq_ups, liq_lows, far = call(
        functools.partial(open_liq, n_liq),
        [cube] * 5 + [(6, cols, width)] + [cube] * 2 + [(2, cols, width)],
        [(2, *cube), (2, 2, cols, width), pltpu.VMEM(cube, jnp.int32)],
        sems=2 * CHUNKS + 2,
        ins=pltpu.HBM,
        limit=OPEN_LIMIT,
    )(liq_rates, dur_rates, upwind)
    alpha, mine, high, less = call(
        open_source, [cube, (8, cols, width)] + [jax.ShapeDtypeStruct((width, width), BF16)] * 2, [flat]
    )(value, utility, income_rates, own, l_inv, l_low, l_before)
    d_inv, d_low, d_before, d_beta, d_gamma, d_mine, dur_ups, dur_lows = call(
        functools.partial(open_dur, n_dur), [turned] * 5 + [(4, rows, width)] + [across_dur] * 2
    )(dur_rates, upwind)
    between = [(i, i + 1) for i in range(1, n_liq - 1, 2)]
    own_coef = other_coef = chip_coefs = None
    for step in range(STEPS):
        final = step == STEPS - 1
        other = swap_liq(mine, 1)
        if step == 0:
            own_coef, other_coef = mine, other
            joint, half = call(join_core, [(6, cols, width), (6, cols // 2, width)])(mine, other, own_coef, other_coef)
            mine_of = named(lambda k: swap_liq(half, 2 * k), n_chips)
            if n_dur == QUAD:
                its = swap_dur(d_mine, 1)
                slope, *d_share = call(pair_weights, [(rows, width), (2, rows, width)])(d_mine, its)
                slope = swap_dur(slope, 2)
                d_coefs = [d_mine, its, slope]
            else:
                d_coefs = [d_mine] + [swap_dur(d_mine, k) for k in range(1, n_dur)]
            its_of = named(lambda k: swap_liq(mine_of[k - 1], 1), n_chips)
            more = [(cols, width), (2, cols, width)] if n_chips == QUAD else []
            mended = call(functools.partial(mend, n_chips - 1), [(6, cols, width)] * (n_chips - 1) + more)(
                joint, *mine_of, *its_of
            )
            chips = [joint, *mended[: n_chips - 1]]
            chip_coefs = chips
        elif n_chips == QUAD:
            joint, sent = call(join_share, [(2, cols, width), (1, cols, width)])(
                mine, other, own_coef, other_coef, mended[-1]
            )
            chips = [joint] + named(lambda k: swap_liq(joint if k == 1 else sent, 2 * k), n_chips)
            chip_coefs = [*chip_coefs[:2], mended[-2]]
        else:
            (joint,) = call(join_core, [(2, cols, width)])(mine, other, own_coef, other_coef)
            chips = [joint] + named(lambda k: swap_liq(joint, 2 * k), n_chips)
        if final:
            *e_lines, e_beta, e_gamma, e_coef = call(
                functools.partial(open_edge, n_dur), [edge] * 5 + [(EDGE, width)], [across_edge] * 2
            )(other_near, far)
        quad, extra = n_dur == QUAD, 2 * EDGE * final
        d_alpha, *outs = call(
            functools.partial(liq_to_dur, n_chips, len(chip_coefs), quad, final),
            [turned, (2 * rows + extra, width)] + [(rows + extra, width)] * quad + [edge] * final,
            [across_dur] + [across_edge] * final,
        )(
            mine, other, own_coef, other_coef, *chips, *chip_coefs, alpha, l_beta, l_gamma, d_inv, d_low, d_before,
            *(d_share if quad else ()), *((*e_lines, e_coef) if final else ()),
        )
        e_alpha = outs[1 + quad :]
        parts = outs[:1] + named(lambda k: swap_dur(outs[int(quad and k > 1)], k), n_dur)
        if step == 0:
            other_near = other
            far = lax.ppermute(far, "liq", between + [(j, i) for i, j in between])
        if not final:
            alpha, mine = call(functools.partial(dur_to_liq, n_dur), [cube, (2, cols, width)], [across_liq, flat])(
                *parts, *d_coefs, d_alpha, d_beta, d_gamma, utility, high, less, l_inv, l_low, l_before
            )
    return call(
        functools.partial(close, n_liq, n_dur),
        [cube, cube],
        [turned_shape(rows + 2, cols, width), across_liq, cube, cube],
        sems=5,
        to=pltpu.HBM,
    )(
        *parts, *d_coefs, d_alpha, d_beta, d_gamma, *e_alpha, e_beta, e_gamma,
        utility, high, less, liq_ups, liq_lows, dur_ups, dur_lows,
    )


def solution(mesh):
    n_liq, n_dur = mesh.shape["liq"], mesh.shape["dur"]
    cell = P("liq", "dur", None)
    pair = P(None, "liq", "dur", None)

    def body(*args):
        return shards(n_liq, n_dur, *args)

    return jax.shard_map(
        body,
        mesh=mesh,
        in_specs=(cell, cell, pair, pair, cell, P()),
        out_specs=(cell, cell),
        check_vma=False,
    )
```
